32 devices in a mesh: dp: 4 (over z), tensor: 8 (over y, x, core).
Axes of the slice: x: 2, y: 2, z: 4, core: 2. Of those that a mesh axis runs over, the one named last changes fastest.
Arguments:
- embed_rows: bfloat16 [98304, 512], P('tensor', 'dp'), may hold values from -6 to 6
- head_rows: bfloat16 [98304, 512], P('tensor', 'dp'), may hold values from -6 to 6
- row_offsets: int32 [2, 9], replicated, may hold values from -2047 to 67583, as said below
- slot_table: int32 [1024], replicated, may hold values from 0 to 1023, as said below
- probe: bfloat16 [512, 1024], replicated, may hold values from -0.25 to 0.25
Outputs:
- stored: bfloat16 [1024, 128, 512], P(('dp', 'tensor'))
- sketch: float32 [1024, 128, 1024], P(('dp', 'tensor'))
The draws below stay inside these ranges and needn't reach their ends.
Inputs may be any that keep to these rules, and one draw needn't show every extreme that they name: row_offsets[m, 8] is row_offsets[m, 0] + 65536; every entry row_offsets[m, t] with t < 8 lies strictly within 2048 rows of t * 8192, and the distance 8192 // 4 - 1 is reached above and below among ranks 1 onward in every row of every draw; row_offsets[m, 0] is never 0, above 0 for one matrix and below 0 for the other. `slot_table`: A permutation of the 1024 block numbers. Devices along dp+tensor write 32 consecutive slots each; among one device's slots exactly 4 blocks come from each aligned range of 8192 vocabulary rows (rows t * 8192 onward of either matrix, both matrices together).
All inputs are finite; a program needn't handle non-finite values.
Results may differ from the reference program's by a relative error of at most 0.001.
Values may be sent and summed in bfloat16 or wider, within the bound.
No kernel may reach another device: no remote copies, remote signals or barrier semaphores. Data moves between devices by JAX's collectives and lax.ppermute only.
A program may use at most 64 MiB of HBM per device.

```python
import jax
import jax.numpy as jnp
from jax import lax

R = 8192
PW = 1024
BLOCK = 128
CAP = 12288
C = 512
NBLK = 512
N_TENSOR = 8
DEVICES = 32


def draw_row_offsets(key, part):
    first, second, third, fourth, fifth = jax.random.split(key, 5)
    reach = R // 4 - 1
    inner = N_TENSOR - 1
    shifts = jax.random.randint(first, (2, inner), -reach, reach + 1)
    upper = jax.random.randint(second, (2,), 0, inner)
    lower = (upper + 1 + jax.random.randint(third, (2,), 0, inner - 1)) % inner
    column = jnp.arange(inner)[None, :]
    shifts = jnp.where(column == upper[:, None], reach, shifts)
    shifts = jnp.where(column == lower[:, None], -reach, shifts)
    interior = jnp.arange(1, N_TENSOR)[None, :] * R + shifts
    size = jax.random.randint(fourth, (2,), 1, reach + 1)
    flip = jax.random.randint(fifth, (), 0, 2)
    signs = jnp.where(jnp.arange(2) == flip, 1, -1)
    starts = (signs * size).astype(jnp.int32)[:, None]
    ends = starts + R * N_TENSOR
    return jnp.concatenate([starts, interior.astype(jnp.int32), ends], axis=1).astype(jnp.int32)


def draw_slot_table(key, part):
    first, second = jax.random.split(key)
    per_rank = R // BLOCK
    total_blocks = per_rank * N_TENSOR
    slot_count = 2 * total_blocks // DEVICES
    shuffled = jax.random.permutation(first, DEVICES).astype(jnp.int32)
    source = (shuffled[:, None] + jnp.arange(slot_count, dtype=jnp.int32)[None, :]) % N_TENSOR
    flat_source = source.reshape(-1)
    slot_total = DEVICES * slot_count
    noise = jax.random.permutation(second, slot_total).astype(jnp.int32)
    ordering = jnp.argsort(flat_source * slot_total + noise)
    within = jnp.arange(slot_total, dtype=jnp.int32) % (2 * per_rank)
    local_block = jnp.zeros((slot_total,), jnp.int32).at[ordering].set(within)
    result = local_block // per_rank * total_blocks + flat_source * per_rank + local_block % per_rank
    return result.astype(jnp.int32)


def steps_of(own_key, extent, pieces, least, high):
    level = 1.0
    for position, parts in pieces:
        draws = jax.random.uniform(jax.random.fold_in(jax.random.fold_in(own_key, 6), position), (parts,), jnp.float32, least / len(pieces), high / len(pieces))
        level = level * jnp.repeat(jnp.exp(draws), extent[position] // parts).reshape((-1,) + (1,) * (len(extent) - 1 - position))
    return level


def normal_values(own_key, extent, scale, bound, cuts=(), kind=jnp.bfloat16):
    gain = steps_of(own_key, extent, cuts, -0.22, 0.18) if cuts else 1.0
    array = jax.random.normal(own_key, extent, jnp.float32) * scale * gain
    return jnp.minimum(jnp.maximum(array, -bound), bound).astype(kind)


def setup_inputs(seed: int = 0) -> dict:
    seeds = jax.random.split(jax.random.key(seed), 6)
    embed_rows = normal_values(seeds[0], (N_TENSOR * CAP, C), 1.0, 6.0, ((0, 8), (1, 4)))
    head_rows = normal_values(seeds[1], (N_TENSOR * CAP, C), 1.0, 6.0, ((0, 8), (1, 4)))
    row_offsets = draw_row_offsets(jax.random.fold_in(seeds[5], 71), 0)
    slot_table = draw_slot_table(jax.random.fold_in(seeds[5], 71), 0)
    probe = normal_values(seeds[4], (C, PW), C ** -0.5, 0.25)
    return dict(embed_rows=embed_rows, head_rows=head_rows, row_offsets=row_offsets, slot_table=slot_table, probe=probe)


def assemble(buffer, offsets):
    vocab_rows = jnp.arange(R * N_TENSOR, dtype=jnp.int32)
    unwrapped = jnp.where(vocab_rows < offsets[0], vocab_rows + R * N_TENSOR,
                          jnp.where(vocab_rows >= offsets[N_TENSOR], vocab_rows - R * N_TENSOR, vocab_rows)).astype(jnp.int32)
    owner = jnp.sum((offsets[1:N_TENSOR][None, :] <= unwrapped[:, None]).astype(jnp.int32), axis=1).astype(jnp.int32)
    source_row = (owner * CAP + unwrapped - offsets[owner]).astype(jnp.int32)
    return buffer[source_row]


def reference(embed_rows, head_rows, row_offsets, slot_table, probe):
    whole = jnp.concatenate([assemble(embed_rows, row_offsets[0]), assemble(head_rows, row_offsets[1])], axis=0)
    blocks = whole.reshape(2 * NBLK, BLOCK, C)
    stored = blocks[slot_table]
    sketch = jnp.dot(stored.reshape(-1, C).astype(jnp.float32), probe.astype(jnp.float32),
                     precision=lax.Precision.HIGHEST, preferred_element_type=jnp.float32)
    return stored, sketch.reshape(2 * NBLK, BLOCK, PW)
```

```python
import functools

import jax
import jax.numpy as jnp
from jax import lax
from jax.experimental import pallas as pl
from jax.experimental.pallas import tpu as pltpu
from jax.sharding import PartitionSpec as P

R = 8192
BLOCK = 128
ALIGN = 16


def from_behind(block, axis, distance):
    devices = range(lax.axis_size(axis))
    route = [((i - distance) % len(devices), i) for i in devices]
    return lax.ppermute(block, axis, route)


def any_space():
    return pl.BlockSpec(memory_space=pl.ANY)


def edges_kernel(starts, embed, head, lead_out, trail_out, rows, wide, sems):
    quarter = lead_out.shape[1]
    raws = [embed, head]
    copies = []
    for m in range(2):
        first = starts[2 + m] // ALIGN * ALIGN
        window = pl.ds(pl.multiple_of(first, ALIGN), quarter + ALIGN)
        lead = pltpu.make_async_copy(
            raws[m].at[pl.ds(0, quarter)], rows.at[2 * m, pl.ds(0, quarter)], sems.at[2 * m]
        )
        trail = pltpu.make_async_copy(raws[m].at[window], rows.at[2 * m + 1], sems.at[2 * m + 1])
        lead.start()
        trail.start()
        copies.append((lead, trail))
    for m in range(2):
        lead, trail = copies[m]
        lead.wait()
        count = starts[m]

        def widen_lead(i, _):
            at = pl.multiple_of(i * BLOCK, BLOCK)
            wide[pl.ds(quarter + at, BLOCK), :] = rows[2 * m, pl.ds(at, BLOCK), :].astype(jnp.float32)
            return _

        lax.fori_loop(0, quarter // BLOCK, widen_lead, 0)

        def put_lead(i, _):
            at = pl.multiple_of(i * BLOCK, BLOCK)
            lead_out[m, pl.ds(at, BLOCK), :] = wide[pl.ds(count + at, BLOCK), :].astype(jnp.bfloat16)
            return _

        lax.fori_loop(0, quarter // BLOCK, put_lead, 0)
        trail.wait()
        shift = starts[2 + m] % ALIGN

        def widen_trail(i, _):
            at = pl.multiple_of(i * BLOCK, BLOCK)
            wide[pl.ds(at, BLOCK), :] = rows[2 * m + 1, pl.ds(at, BLOCK), :].astype(jnp.float32)
            return _

        lax.fori_loop(0, quarter // BLOCK, widen_trail, 0)
        wide[pl.ds(quarter, ALIGN), :] = rows[2 * m + 1, pl.ds(quarter, ALIGN), :].astype(jnp.float32)

        def put_trail(i, _):
            at = pl.multiple_of(i * BLOCK, BLOCK)
            trail_out[m, pl.ds(at, BLOCK), :] = wide[pl.ds(shift + at, BLOCK), :].astype(jnp.bfloat16)
            return _

        lax.fori_loop(0, quarter // BLOCK, put_trail, 0)


def cut_edges(embed, head, n_lead, tail_begin, quarter):
    width = embed.shape[1]
    starts = jnp.concatenate([n_lead, tail_begin])
    shape = jax.ShapeDtypeStruct((2, quarter, width), embed.dtype)
    return pl.pallas_call(
        edges_kernel,
        out_shape=(shape, shape),
        in_specs=[pl.BlockSpec(memory_space=pltpu.SMEM), any_space(), any_space()],
        out_specs=[pl.BlockSpec(memory_space=pltpu.VMEM)] * 2,
        scratch_shapes=[
            pltpu.VMEM((4, quarter + ALIGN, width), embed.dtype),
            pltpu.VMEM((2 * quarter, width), jnp.float32),
            pltpu.SemaphoreType.DMA((4,)),
        ],
    )(starts, embed, head)


def pack_kernel(picked, before, embed, head, *refs):
    outs, (rows, wide, sems) = refs[:-3], refs[-3:]
    height = embed.shape[0]
    per_rank = R // BLOCK
    copies = []
    for m, raw in enumerate([embed, head]):
        copy = pltpu.make_async_copy(
            raw, rows.at[pl.ds(BLOCK + m * height, height)], sems.at[m]
        )
        copy.start()
        copies.append(copy)
    for copy in copies:
        copy.wait()
    per_piece = outs[0].shape[0]
    for c, out in enumerate(outs):

        def body(d, _):
            block = picked[c * per_piece + d]
            m = block // per_rank
            start = block % per_rank * BLOCK - before[m]
            start = jnp.maximum(start + BLOCK, 0) + m * height
            first = pl.multiple_of(start // ALIGN * ALIGN, ALIGN)
            slot = lax.rem(d, 2)
            wide[slot] = rows[pl.ds(first, BLOCK + ALIGN), :].astype(jnp.float32)
            out[d] = wide[slot, pl.ds(start - first, BLOCK), :].astype(jnp.bfloat16)
            return _

        lax.fori_loop(0, per_piece, body, 0)


def pack_local(picked, before, embed, head, pieces, per_piece):
    height, width = embed.shape
    shape = jax.ShapeDtypeStruct((per_piece, BLOCK, width), embed.dtype)
    smem = pl.BlockSpec(memory_space=pltpu.SMEM)
    return pl.pallas_call(
        pack_kernel,
        out_shape=[shape] * pieces,
        in_specs=[smem, smem, any_space(), any_space()],
        out_specs=[pl.BlockSpec(memory_space=pltpu.VMEM)] * pieces,
        scratch_shapes=[
            pltpu.VMEM((BLOCK + 2 * height, width), embed.dtype),
            pltpu.VMEM((2, BLOCK + ALIGN, width), jnp.float32),
            pltpu.SemaphoreType.DMA((2,)),
        ],
        cost_estimate=pl.CostEstimate(flops=4_000_000_000, bytes_accessed=10_000_000, transcendentals=0),
    )(picked, before, embed, head)


def overlay_kernel(picked, before, after, packed, left, right, out):
    per_rank = R // BLOCK
    quarter = left.shape[1]

    def body(d, _):
        block = picked[d]
        m = block // per_rank
        first = block % per_rank * BLOCK
        out[d] = packed[d]
        row = first + lax.broadcasted_iota(jnp.int32, (BLOCK, 1), 0)

        @pl.when(first < before[m])
        def _left():
            at = pl.multiple_of(first, BLOCK)
            out[d] = jnp.where(row < before[m], left[m, pl.ds(at, BLOCK), :], out[d])

        @pl.when(first + BLOCK > after[m])
        def _right():
            at = pl.multiple_of(first - (R - quarter), BLOCK)
            out[d] = jnp.where(row >= after[m], right[m, pl.ds(at, BLOCK), :], out[d])

        return _

    lax.fori_loop(0, packed.shape[0], body, 0)


def overlay(picked, before, after, packed, left, right):
    smem = pl.BlockSpec(memory_space=pltpu.SMEM)
    vmem = pl.BlockSpec(memory_space=pltpu.VMEM)
    return pl.pallas_call(
        overlay_kernel,
        out_shape=jax.ShapeDtypeStruct(packed.shape, packed.dtype),
        in_specs=[smem] * 3 + [vmem] * 3,
        out_specs=vmem,
        cost_estimate=pl.CostEstimate(flops=1_000_000_000, bytes_accessed=4_000_000, transcendentals=0),
    )(picked, before, after, packed, left, right)


def store_kernel(position, incoming, probe, *refs):
    stored, sketch = refs[-2:]
    n_data, width = incoming.shape[0], incoming.shape[3]
    for z in range(n_data):
        stored[0, :, z * width : (z + 1) * width] = incoming[z, 0]
    sketch[0] = jnp.dot(stored[0], probe[...], preferred_element_type=jnp.float32)


def store_piece(position, incoming, probe, slot_count, previous):
    n_data, n_tensor, _, width = incoming.shape
    columns = n_data * width
    sketch_width = probe.shape[1]
    out_shape = [
        jax.ShapeDtypeStruct((slot_count, BLOCK, columns), incoming.dtype),
        jax.ShapeDtypeStruct((slot_count, BLOCK, sketch_width), jnp.float32),
    ]
    held = [] if previous is None else list(previous)
    return pl.pallas_call(
        store_kernel,
        out_shape=out_shape,
        grid_spec=pltpu.PrefetchScalarGridSpec(
            num_scalar_prefetch=1,
            grid=(n_tensor,),
            in_specs=[
                pl.BlockSpec((n_data, 1, BLOCK, width), lambda i, p: (0, i, 0, 0)),
                pl.BlockSpec((columns, sketch_width), lambda i, p: (0, 0)),
            ]
            + [any_space() for _ in held],
            out_specs=[
                pl.BlockSpec((1, BLOCK, columns), lambda i, p: (p[i], 0, 0)),
                pl.BlockSpec((1, BLOCK, sketch_width), lambda i, p: (p[i], 0, 0)),
            ],
        ),
        input_output_aliases={3: 0, 4: 1} if held else {},
        cost_estimate=pl.CostEstimate(
            flops=2 * n_tensor * BLOCK * columns * sketch_width,
            bytes_accessed=6_000_000,
            transcendentals=0,
        ),
    )(position, incoming, probe, *held)


def shards(embed_rows, head_rows, row_offsets, slot_table, probe):
    n_tensor = lax.axis_size("tensor")
    n_data = lax.axis_size("dp")
    my_tensor = lax.axis_index("tensor")
    my_data = lax.axis_index("dp")
    quarter = R // 4
    col_width = embed_rows.shape[1]
    devices = n_tensor * n_data
    per_rank = R // BLOCK
    total_blocks = per_rank * n_tensor
    slot_count = 2 * total_blocks // devices
    max_from = slot_count // n_tensor

    mine = lax.dynamic_slice_in_dim(row_offsets, my_tensor, 2, 1)
    before = mine[:, 0] - my_tensor * R
    after = mine[:, 1] - my_tensor * R
    n_lead = jnp.clip(-before, 0, quarter)
    tail_begin = R - before
    lead_part, trail_part = cut_edges(embed_rows, head_rows, n_lead, tail_begin, quarter)
    from_right = from_behind(lead_part, "tensor", -1)
    from_left = from_behind(trail_part, "tensor", 1)

    slot_grid = slot_table.reshape(devices, slot_count)
    source = slot_grid % total_blocks // per_rank
    local_block = slot_grid // total_blocks * per_rank + slot_grid % per_rank
    from_me = source == my_tensor
    rank_order = jnp.cumsum(from_me.astype(jnp.int32), axis=1) - 1
    slot_index = jnp.arange(max_from, dtype=jnp.int32)
    select = from_me[:, None, :] & (rank_order[:, None, :] == slot_index[None, :, None])
    picked = jnp.sum(jnp.where(select, local_block[:, None, :], 0), axis=2).T
    packed = pack_local(picked.reshape(-1), before, embed_rows, head_rows, max_from, devices)

    writer = my_data * n_tensor + my_tensor
    my_source = lax.dynamic_slice_in_dim(source, writer, 1, 0)[0]
    slot_range = jnp.arange(slot_count, dtype=jnp.int32)
    earlier = (my_source[None, :] == my_source[:, None]) & (
        slot_range[None, :] < slot_range[:, None]
    )
    rank_within = jnp.sum(earlier.astype(jnp.int32), axis=1)
    order = rank_within * n_tensor + my_source
    position = jnp.sum(
        jnp.where(order[None, :] == slot_range[:, None], slot_range[None, :], 0), axis=1
    ).reshape(max_from, n_tensor)

    outputs = None
    for c in range(max_from):
        outgoing = overlay(picked[c], before, after, packed[c], from_left, from_right)
        incoming = lax.all_to_all(
            outgoing, ("dp", "tensor"), split_axis=0, concat_axis=0, tiled=True
        )
        incoming = incoming.reshape(n_data, n_tensor, BLOCK, col_width)
        outputs = store_piece(position[c], incoming, probe, slot_count, outputs)
    return tuple(outputs)


def solution(mesh):
    return jax.shard_map(
        shards,
        mesh=mesh,
        in_specs=(P("tensor", "dp"), P("tensor", "dp"), P(), P(), P()),
        out_specs=(P(("dp", "tensor"), None, None), P(("dp", "tensor"), None, None)),
        check_vma=False,
    )
```

```python
import functools

import jax
import jax.numpy as jnp
from jax import lax
from jax.experimental import pallas as pl
from jax.experimental.pallas import tpu as pltpu
from jax.sharding import PartitionSpec as P


R = 8192
BLOCK = 128
ALIGN = 16
MIB = 1 << 20


def from_behind(block, axis, distance):
    devices = range(lax.axis_size(axis))
    route = [((i - distance) % len(devices), i) for i in devices]
    return lax.ppermute(block, axis, route)


def any_space():
    return pl.BlockSpec(memory_space=pl.ANY)


def in_hbm():
    return pl.BlockSpec(memory_space=pltpu.HBM)


def smem():
    return pl.BlockSpec(memory_space=pltpu.SMEM)


def vmem():
    return pl.BlockSpec(memory_space=pltpu.VMEM)


def my_span(offsets, m):
    t = lax.axis_index("tensor")
    return offsets[m, t] - t * R, offsets[m, t + 1] - t * R


def edges_kernel(offsets, embed, head, lead_out, trail_out, rows, wide, sems):
    quarter = lead_out.shape[1]
    raws = [embed, head]
    copies = []
    for m in range(2):
        first = (R - my_span(offsets, m)[0]) // ALIGN * ALIGN
        window = pl.ds(pl.multiple_of(first, ALIGN), quarter + ALIGN)
        lead = pltpu.make_async_copy(
            raws[m].at[pl.ds(0, quarter)], rows.at[2 * m, pl.ds(0, quarter)], sems.at[2 * m]
        )
        trail = pltpu.make_async_copy(raws[m].at[window], rows.at[2 * m + 1], sems.at[2 * m + 1])
        lead.start()
        trail.start()
        copies.append((lead, trail))
    for m in range(2):
        lead, trail = copies[m]
        lead.wait()
        before = my_span(offsets, m)[0]
        count = jnp.clip(-before, 0, quarter)

        def widen_lead(i, _):
            at = pl.multiple_of(i * BLOCK, BLOCK)
            wide[pl.ds(quarter + at, BLOCK), :] = rows[2 * m, pl.ds(at, BLOCK), :].astype(jnp.float32)
            return _

        lax.fori_loop(0, quarter // BLOCK, widen_lead, 0)

        def put_lead(i, _):
            at = pl.multiple_of(i * BLOCK, BLOCK)
            lead_out[m, pl.ds(at, BLOCK), :] = wide[pl.ds(count + at, BLOCK), :].astype(jnp.bfloat16)
            return _

        lax.fori_loop(0, quarter // BLOCK, put_lead, 0)
        trail.wait()
        shift = (R - before) % ALIGN

        def widen_trail(i, _):
            at = pl.multiple_of(i * BLOCK, BLOCK)
            wide[pl.ds(at, BLOCK), :] = rows[2 * m + 1, pl.ds(at, BLOCK), :].astype(jnp.float32)
            return _

        lax.fori_loop(0, quarter // BLOCK, widen_trail, 0)
        wide[pl.ds(quarter, ALIGN), :] = rows[2 * m + 1, pl.ds(quarter, ALIGN), :].astype(jnp.float32)

        def put_trail(i, _):
            at = pl.multiple_of(i * BLOCK, BLOCK)
            trail_out[m, pl.ds(at, BLOCK), :] = wide[pl.ds(shift + at, BLOCK), :].astype(jnp.bfloat16)
            return _

        lax.fori_loop(0, quarter // BLOCK, put_trail, 0)


def cut_edges(offsets, embed, head, quarter):
    width = embed.shape[1]
    shape = jax.ShapeDtypeStruct((2, quarter, width), embed.dtype)
    return pl.pallas_call(
        edges_kernel,
        out_shape=(shape, shape),
        in_specs=[smem(), in_hbm(), in_hbm()],
        out_specs=[vmem()] * 2,
        scratch_shapes=[
            pltpu.VMEM((4, quarter + ALIGN, width), embed.dtype),
            pltpu.VMEM((2 * quarter, width), jnp.float32),
            pltpu.SemaphoreType.DMA((4,)),
        ],
        compiler_params=pltpu.CompilerParams(vmem_limit_bytes=61 * MIB),
    )(offsets, embed, head)


def target_of(step, n_data, n_tensor):
    z = lax.rem(lax.axis_index("dp") + step % n_data, n_data)
    t = lax.rem(lax.axis_index("tensor") + step // n_data, n_tensor)
    return z * n_tensor + t


def pack_kernel(n_data, n_tensor, picked, offsets, embed, head, *refs):
    outs, (rows, wide, sems) = refs[:-3], refs[-3:]
    height = embed.shape[0]
    per_rank = R // BLOCK
    copies = []
    for m, raw in enumerate([embed, head]):
        copy = pltpu.make_async_copy(
            raw, rows.at[pl.ds(BLOCK + m * height, height)], sems.at[m]
        )
        copy.start()
        copies.append(copy)
    for copy in copies:
        copy.wait()
    per_pair = picked.shape[1]
    step = 0
    for out in outs:

        def body(i, _, step=step, out=out):
            block = picked[target_of(step + i // per_pair, n_data, n_tensor), i % per_pair]
            m = block // per_rank
            start = block % per_rank * BLOCK - my_span(offsets, m)[0]
            start = jnp.maximum(start + BLOCK, 0) + m * height
            first = pl.multiple_of(start // ALIGN * ALIGN, ALIGN)
            slot = lax.rem(i, 2)
            wide[slot] = rows[pl.ds(first, BLOCK + ALIGN), :].astype(jnp.float32)
            out[i] = wide[slot, pl.ds(start - first, BLOCK), :].astype(jnp.bfloat16)
            return _

        lax.fori_loop(0, out.shape[0], body, 0)
        step += out.shape[0] // per_pair


def pack_local(picked, offsets, embed, head, groups, n_data, n_tensor):
    height, width = embed.shape
    return pl.pallas_call(
        functools.partial(pack_kernel, n_data, n_tensor),
        out_shape=[
            jax.ShapeDtypeStruct((count, BLOCK, width), embed.dtype) for count in groups
        ],
        in_specs=[smem(), smem(), in_hbm(), in_hbm()],
        out_specs=[vmem()] * len(groups),
        scratch_shapes=[
            pltpu.VMEM((BLOCK + 2 * height, width), embed.dtype),
            pltpu.VMEM((2, BLOCK + ALIGN, width), jnp.float32),
            pltpu.SemaphoreType.DMA((2,)),
        ],
        compiler_params=pltpu.CompilerParams(vmem_limit_bytes=16 * MIB),
        cost_estimate=pl.CostEstimate(flops=4_000_000_000, bytes_accessed=10_000_000, transcendentals=0),
    )(picked, offsets, embed, head)


def overlay_kernel(first_step, n_data, n_tensor, picked, offsets, packed, left, right, *outs):
    per_rank = R // BLOCK
    quarter = left.shape[1]
    per_pair = picked.shape[1]
    for k, out in enumerate(outs):
        target = target_of(first_step + k, n_data, n_tensor)

        def body(j, _, k=k, out=out, target=target):
            block = picked[target, j]
            m = block // per_rank
            before, after = my_span(offsets, m)
            first = block % per_rank * BLOCK
            out[j] = packed[k * per_pair + j]
            row = first + lax.broadcasted_iota(jnp.int32, (BLOCK, 1), 0)

            @pl.when(first < before)
            def _left():
                at = pl.multiple_of(first, BLOCK)
                out[j] = jnp.where(row < before, left[m, pl.ds(at, BLOCK), :], out[j])

            @pl.when(first + BLOCK > after)
            def _right():
                at = pl.multiple_of(first - (R - quarter), BLOCK)
                out[j] = jnp.where(row >= after, right[m, pl.ds(at, BLOCK), :], out[j])

            return _

        lax.fori_loop(0, per_pair, body, 0)


def overlay(first_step, picked, offsets, packed, left, right, n_data, n_tensor):
    per_pair = picked.shape[1]
    steps = packed.shape[0] // per_pair
    return pl.pallas_call(
        functools.partial(overlay_kernel, first_step, n_data, n_tensor),
        out_shape=[jax.ShapeDtypeStruct((per_pair,) + packed.shape[1:], packed.dtype)] * steps,
        in_specs=[smem()] * 2 + [vmem()] * 3,
        out_specs=[vmem()] * steps,
        compiler_params=pltpu.CompilerParams(vmem_limit_bytes=16 * MIB),
        cost_estimate=pl.CostEstimate(flops=1_000_000_000, bytes_accessed=4_000_000, transcendentals=0),
    )(picked, offsets, packed, left, right)


def store_kernel(n_data, position, *refs):
    incoming, probe = refs[:n_data], refs[n_data]
    stored, sketch, full, product, sems = refs[-5:]
    per_pair, _, width = incoming[0].shape
    for s in range(n_data):
        column = pl.multiple_of(lax.rem(lax.axis_index("dp") - s + n_data, n_data) * width, width)
        for j in range(per_pair):
            full[j, :, pl.ds(column, width)] = incoming[s][j]
    copies = []
    for j in range(per_pair):
        product[j] = jnp.dot(full[j], probe[...], preferred_element_type=jnp.float32)
        slot = position[j]
        copies.append(pltpu.make_async_copy(full.at[j], stored.at[slot], sems.at[2 * j]))
        copies.append(pltpu.make_async_copy(product.at[j], sketch.at[slot], sems.at[2 * j + 1]))
        copies[-2].start()
        copies[-1].start()
    for copy in copies:
        copy.wait()


def store_group(position, incoming, probe, slot_count, previous):
    n_data = len(incoming)
    per_pair, _, width = incoming[0].shape
    columns = n_data * width
    sketch_width = probe.shape[1]
    out_shape = [
        jax.ShapeDtypeStruct((slot_count, BLOCK, columns), incoming[0].dtype),
        jax.ShapeDtypeStruct((slot_count, BLOCK, sketch_width), jnp.float32),
    ]
    held = [] if previous is None else list(previous)
    at = 2 + n_data
    return pl.pallas_call(
        functools.partial(store_kernel, n_data),
        out_shape=out_shape,
        in_specs=[smem()] + [vmem()] * (n_data + 1) + [any_space() for _ in held],
        out_specs=[any_space(), any_space()],
        scratch_shapes=[
            pltpu.VMEM((per_pair, BLOCK, columns), incoming[0].dtype),
            pltpu.VMEM((per_pair, BLOCK, sketch_width), jnp.float32),
            pltpu.SemaphoreType.DMA((2 * per_pair,)),
        ],
        compiler_params=pltpu.CompilerParams(vmem_limit_bytes=10 * MIB),
        input_output_aliases={at: 0, at + 1: 1} if held else {},
        cost_estimate=pl.CostEstimate(
            flops=2 * per_pair * BLOCK * columns * sketch_width,
            bytes_accessed=4_000_000,
            transcendentals=0,
        ),
    )(position, *incoming, probe, *held)


def shards(embed_rows, head_rows, row_offsets, slot_table, probe):
    n_tensor = lax.axis_size("tensor")
    n_data = lax.axis_size("dp")
    my_tensor = lax.axis_index("tensor")
    my_data = lax.axis_index("dp")
    quarter = R // 4
    devices = n_tensor * n_data
    per_rank = R // BLOCK
    total_blocks = per_rank * n_tensor
    slot_count = 2 * total_blocks // devices
    per_pair = slot_count // n_tensor
    lead_part, trail_part = cut_edges(row_offsets, embed_rows, head_rows, quarter)
    from_right = from_behind(lead_part, "tensor", -1)
    from_left = from_behind(trail_part, "tensor", 1)

    slot_grid = slot_table.reshape(devices, slot_count)
    source = slot_grid % total_blocks // per_rank
    local_block = slot_grid // total_blocks * per_rank + slot_grid % per_rank
    from_me = source == my_tensor
    rank_order = jnp.cumsum(from_me.astype(jnp.int32), axis=1) - 1
    slot_index = jnp.arange(per_pair, dtype=jnp.int32)
    select = from_me[:, None, :] & (rank_order[:, None, :] == slot_index[None, :, None])
    picked = jnp.sum(jnp.where(select, local_block[:, None, :], 0), axis=2)

    writer = my_data * n_tensor + my_tensor
    my_source = lax.dynamic_slice_in_dim(source, writer, 1, 0)[0]
    slot_range = jnp.arange(slot_count, dtype=jnp.int32)
    earlier = (my_source[None, :] == my_source[:, None]) & (
        slot_range[None, :] < slot_range[:, None]
    )
    rank_within = jnp.sum(earlier.astype(jnp.int32), axis=1)
    hops = (my_tensor - my_source + n_tensor) % n_tensor
    order = hops * per_pair + rank_within
    position = jnp.sum(
        jnp.where(order[None, :] == slot_range[:, None], slot_range[None, :], 0), axis=1
    ).reshape(n_tensor, per_pair)

    def move(block, step):
        u, s = step // n_data, step % n_data
        route = []
        for z in range(n_data):
            for t in range(n_tensor):
                to = (z + s) % n_data * n_tensor + (t + u) % n_tensor
                route.append((z * n_tensor + t, to))
        if not step:
            return block
        return lax.ppermute(block, ("dp", "tensor"), route)

    groups = [n_data * per_pair, (devices - n_data) * per_pair]
    packed = pack_local(picked, row_offsets, embed_rows, head_rows, groups, n_data, n_tensor)
    outgoing = []
    for k, first_step in enumerate([0, n_data]):
        outgoing += overlay(
            first_step, picked, row_offsets, packed[k], from_left, from_right, n_data, n_tensor
        )
    outputs = None
    for u in range(n_tensor):
        incoming = [move(outgoing[u * n_data + s], u * n_data + s) for s in range(n_data)]
        outputs = store_group(position[u], incoming, probe, slot_count, outputs)
    return tuple(outputs)


def solution(mesh):
    return jax.shard_map(
        shards,
        mesh=mesh,
        in_specs=(P("tensor", "dp"), P("tensor", "dp"), P(), P(), P()),
        out_specs=(P(("dp", "tensor"), None, None), P(("dp", "tensor"), None, None)),
        check_vma=False,
    )
```

```python
import functools

import jax
import jax.numpy as jnp
from jax import lax
from jax.experimental import pallas as pl
from jax.experimental.pallas import tpu as pltpu
from jax.sharding import PartitionSpec as P


R = 8192
BLOCK = 128
LATE = 1
DIRECT = 2
ALIGN = 16
MIB = 1 << 20


def from_behind(block, axis, distance):
    devices = range(lax.axis_size(axis))
    route = [((i - distance) % len(devices), i) for i in devices]
    return lax.ppermute(block, axis, route)


def any_space():
    return pl.BlockSpec(memory_space=pl.ANY)


def in_hbm():
    return pl.BlockSpec(memory_space=pltpu.HBM)


def smem():
    return pl.BlockSpec(memory_space=pltpu.SMEM)


def vmem():
    return pl.BlockSpec(memory_space=pltpu.VMEM)


def my_span(offsets, m):
    t = lax.axis_index("tensor")
    return offsets[m, t] - t * R, offsets[m, t + 1] - t * R


def edges_kernel(offsets, embed, head, lead_out, trail_out, rows, wide, sems):
    quarter = lead_out.shape[1]
    raws = [embed, head]
    copies = []
    for m in range(2):
        first = (R - my_span(offsets, m)[0]) & -ALIGN
        window = pl.ds(pl.multiple_of(first, ALIGN), quarter + ALIGN)
        lead = pltpu.make_async_copy(
            raws[m].at[pl.ds(0, quarter)], rows.at[2 * m, pl.ds(0, quarter)], sems.at[2 * m]
        )
        trail = pltpu.make_async_copy(raws[m].at[window], rows.at[2 * m + 1], sems.at[2 * m + 1])
        lead.start()
        trail.start()
        copies.append((lead, trail))
    blocks = quarter // BLOCK
    for m in range(2):
        lead, trail = copies[m]
        before, after = my_span(offsets, m)
        lead.wait()
        count = jnp.clip(-before, 0, quarter)
        used = (count + BLOCK - 1) >> log2(BLOCK)

        def widen_lead(i, _):
            at = pl.multiple_of(i * BLOCK, BLOCK)
            wide[pl.ds(quarter + at, BLOCK), :] = rows[2 * m, pl.ds(at, BLOCK), :].astype(jnp.float32)
            return _

        lax.fori_loop(0, used, widen_lead, 0)

        def put_lead(i, _):
            at = pl.multiple_of(i * BLOCK, BLOCK)
            lead_out[m, pl.ds(at, BLOCK), :] = wide[pl.ds(count + at, BLOCK), :].astype(jnp.bfloat16)
            return _

        lax.fori_loop(blocks - used, blocks, put_lead, 0)
        trail.wait()
        shift = (R - before) & (ALIGN - 1)
        used = (jnp.clip(after - R, 0, quarter) + BLOCK - 1) >> log2(BLOCK)

        def widen_trail(i, _):
            at = pl.multiple_of(i * BLOCK, BLOCK)
            wide[pl.ds(at, BLOCK), :] = rows[2 * m + 1, pl.ds(at, BLOCK), :].astype(jnp.float32)
            return _

        lax.fori_loop(0, jnp.minimum(used + 1, blocks), widen_trail, 0)

        @pl.when(used == blocks)
        def _last():
            wide[pl.ds(quarter, ALIGN), :] = rows[2 * m + 1, pl.ds(quarter, ALIGN), :].astype(jnp.float32)

        def put_trail(i, _):
            at = pl.multiple_of(i * BLOCK, BLOCK)
            trail_out[m, pl.ds(at, BLOCK), :] = wide[pl.ds(shift + at, BLOCK), :].astype(jnp.bfloat16)
            return _

        lax.fori_loop(0, used, put_trail, 0)


def cut_edges(offsets, embed, head, quarter):
    width = embed.shape[1]
    shape = jax.ShapeDtypeStruct((2, quarter, width), embed.dtype)
    return pl.pallas_call(
        edges_kernel,
        out_shape=(shape, shape),
        in_specs=[smem(), in_hbm(), in_hbm()],
        out_specs=[vmem()] * 2,
        scratch_shapes=[
            pltpu.VMEM((4, quarter + ALIGN, width), embed.dtype),
            pltpu.VMEM((2 * quarter, width), jnp.float32),
            pltpu.SemaphoreType.DMA((4,)),
        ],
        compiler_params=pltpu.CompilerParams(vmem_limit_bytes=61 * MIB),
    )(offsets, embed, head)


def log2(size):
    assert size & (size - 1) == 0
    return size.bit_length() - 1


def wrap(index, size):
    return index & (size - 1)


def target(s, u, n_data, n_tensor):
    z = wrap(lax.axis_index("dp") + s, n_data)
    t = wrap(lax.axis_index("tensor") + u, n_tensor)
    return z * n_tensor + t


def split_block(block):
    bits = log2(R // BLOCK)
    return block >> bits, (block & (R // BLOCK - 1)) * BLOCK


def plan_kernel(n_data, n_tensor, per_pair, offsets, slots, plan):
    devices, count = slots.shape
    per_rank = R // BLOCK
    total = per_rank * n_tensor
    slot = slots[...]
    matrix = slot >> log2(total)
    rest = slot & (total - 1)
    source = rest >> log2(per_rank)
    k = rest & (per_rank - 1)
    local = jnp.zeros_like(slot)
    for m in range(2):
        for t in range(n_tensor):
            begin = offsets[m, t] - t * R
            end = offsets[m, t + 1] - t * R
            inside = (k * BLOCK >= begin) & (k * BLOCK + BLOCK <= end)
            here = (source == t) & (matrix == m)
            local = jnp.where(here & inside, 1, local)
    column = lax.broadcasted_iota(jnp.int32, slot.shape, 1)
    lowest = source * (2 * count)
    key = lowest + (1 - local) * count + column
    rank = jnp.zeros_like(slot)
    for j in range(count):
        other = key[:, j : j + 1]
        rank += jnp.where((other >= lowest) & (other < key), 1, 0)
    my_t = lax.axis_index("tensor")
    me = lax.axis_index("dp") * n_tensor + my_t
    lane = lax.broadcasted_iota(jnp.int32, plan.shape, 1)
    row = lax.broadcasted_iota(jnp.int32, slot.shape, 0)
    out = jnp.zeros(plan.shape, jnp.int32)
    block = matrix * per_rank + k
    for r in range(per_pair):
        mine = (source == my_t) & (rank == r)
        picked = jnp.sum(jnp.where(mine, block, 0), axis=1, keepdims=True)
        out = jnp.where(lane == r, picked, out)
        if r == 0:
            flag = jnp.sum(jnp.where(mine, local, 0), axis=1, keepdims=True)
            out = jnp.where(lane == per_pair, flag, out)
    hops = (my_t - source) & (n_tensor - 1)
    order = jnp.where(row == me, hops * per_pair + rank, 0)
    order = jnp.sum(order, axis=0, keepdims=True)
    found = jnp.where(order == row, column, 0)
    out = jnp.where(lane == per_pair + 1, jnp.sum(found, axis=1, keepdims=True), out)
    empty = jnp.zeros(plan.shape, jnp.int32)
    for t in range(n_tensor):
        has = jnp.max(jnp.where(source == t, local, 0), axis=1, keepdims=True)
        empty = jnp.where(lane == t, 1 - has, empty)
    worst = jnp.zeros((1, 1), jnp.int32)
    for z in range(n_data):
        layer = jnp.sum(empty[z * n_tensor : (z + 1) * n_tensor], axis=0, keepdims=True)
        worst = jnp.maximum(worst, jnp.max(layer, axis=1, keepdims=True))
    plan[...] = jnp.where(lane == per_pair + 2, worst, out)


def make_plan(offsets, slot_table, n_data, n_tensor, per_pair):
    devices = n_data * n_tensor
    return pl.pallas_call(
        functools.partial(plan_kernel, n_data, n_tensor, per_pair),
        out_shape=jax.ShapeDtypeStruct((devices, 128), jnp.int32),
        in_specs=[smem(), vmem()],
        out_specs=vmem(),
        compiler_params=pltpu.CompilerParams(vmem_limit_bytes=4 * MIB),
    )(offsets, slot_table.reshape(devices, -1))


class Layout:
    def __init__(self, n_data, n_tensor, per_pair):
        self.n_data, self.n_tensor, self.per_pair = n_data, n_tensor, per_pair
        self.staged = per_pair > DIRECT + 1
        self.direct_ranks = DIRECT if self.staged else per_pair

    def target(self, s, u):
        return target(s, u, self.n_data, self.n_tensor)

    def along_z(self, s, rank):
        return (0, self.n_tensor, lambda plan, i: plan[self.target(s, i), rank])

    def late_block(self, plan, s):
        chosen = self.target(s, 0)
        for u in reversed(range(self.n_tensor)):
            to = self.target(s, u)
            chosen = jnp.where(plan[to, self.per_pair] == 0, to, chosen)
        return plan[chosen, 0]

    def late(self):
        return [
            [(0, LATE, lambda plan, i, s=s: self.late_block(plan, s))] for s in range(self.n_data)
        ]

    def stage(self, rank):
        return [[self.along_z(s, rank)] for s in range(self.n_data)]

    def direct(self):
        count, first = self.direct_ranks, self.per_pair - self.direct_ranks
        bits = log2(count)
        which = lambda plan, i: plan[i >> bits, first + (i & (count - 1))]
        return [[(0, self.n_data * self.n_tensor * count, which)]]

    def size(self, parts):
        return sum(part[1] for part in parts)


def pack_kernel(arrays, plan, offsets, embed, head, *refs):
    outs, (windows, wide, sems) = refs[: len(arrays)], refs[len(arrays) :]
    height = embed.shape[0]

    t = lax.axis_index("tensor")
    begins = [offsets[m, t] - t * R for m in range(2)]

    def where_from(block):
        m, row = split_block(block)
        start = row - jnp.where(m == 0, begins[0], begins[1])
        start = jnp.minimum(jnp.maximum(start + BLOCK, 0), height - ALIGN)
        first = jnp.maximum((start & -ALIGN) - BLOCK, 0)
        return m, start - BLOCK, pl.multiple_of(first, ALIGN)

    at = 0
    for parts in arrays:
        for begin, count, which in parts:

            def fetch(i, _, at=at, which=which):
                m, _start, first = where_from(which(plan, i))
                for k, raw in enumerate([embed, head]):

                    @pl.when(m == k)
                    def _fetch(raw=raw):
                        pltpu.make_async_copy(
                            raw.at[pl.ds(first, BLOCK + ALIGN)], windows.at[at + i], sems.at[at + i]
                        ).start()

                return _

            lax.fori_loop(0, count, fetch, 0)
            at += count
    at = 0
    for parts, out in zip(arrays, outs):
        for begin, count, which in parts:

            def shift(i, _, at=at, which=which, out=out, begin=begin):
                m, start, first = where_from(which(plan, i))
                pltpu.make_async_copy(
                    embed.at[pl.ds(0, BLOCK + ALIGN)], windows.at[at + i], sems.at[at + i]
                ).wait()
                slot = i & 1
                wide[slot, pl.ds(BLOCK, BLOCK + ALIGN), :] = windows[at + i].astype(jnp.float32)
                moved = wide[slot, pl.ds(BLOCK + start - first, BLOCK), :]
                out[begin + i] = moved.astype(jnp.bfloat16)
                return _

            lax.fori_loop(0, count, shift, 0)
            at += count


def pack(layout, arrays, plan, offsets, embed, head, limit):
    width = embed.shape[1]
    total = sum(layout.size(parts) for parts in arrays)
    return pl.pallas_call(
        functools.partial(pack_kernel, arrays),
        out_shape=[
            jax.ShapeDtypeStruct((layout.size(parts), BLOCK, width), embed.dtype) for parts in arrays
        ],
        in_specs=[smem(), smem(), in_hbm(), in_hbm()],
        out_specs=[vmem()] * len(arrays),
        scratch_shapes=[
            pltpu.VMEM((total, BLOCK + ALIGN, width), embed.dtype),
            pltpu.VMEM((2, 2 * BLOCK + ALIGN, width), jnp.float32),
            pltpu.SemaphoreType.DMA((total,)),
        ],
        compiler_params=pltpu.CompilerParams(vmem_limit_bytes=limit * MIB),
        cost_estimate=pl.CostEstimate(flops=total * 30_000_000, bytes_accessed=total * 70_000, transcendentals=0),
    )(plan, offsets, embed, head)


def overlay_kernel(arrays, plan, offsets, *refs):
    packed, left, right, outs = refs[: len(arrays)], refs[-len(arrays) - 2], refs[-len(arrays) - 1], refs[-len(arrays) :]
    quarter = left.shape[1]
    t = lax.axis_index("tensor")
    begins = [offsets[m, t] - t * R for m in range(2)]
    ends = [offsets[m, t + 1] - t * R for m in range(2)]
    for parts, source, out in zip(arrays, packed, outs):
        out[...] = source[...]
        for begin, count, which in parts:

            def fix(i, _, begin=begin, which=which, out=out):
                m, first = split_block(which(plan, i))
                before = jnp.where(m == 0, begins[0], begins[1])
                after = jnp.where(m == 0, ends[0], ends[1])

                @pl.when(first < before)
                def _left():
                    row = first + lax.broadcasted_iota(jnp.int32, (BLOCK, 1), 0)
                    edge = left[m, pl.ds(pl.multiple_of(first, BLOCK), BLOCK), :]
                    out[begin + i] = jnp.where(row < before, edge, out[begin + i])

                @pl.when(first + BLOCK > after)
                def _right():
                    row = first + lax.broadcasted_iota(jnp.int32, (BLOCK, 1), 0)
                    at = pl.multiple_of(first - (R - quarter), BLOCK)
                    edge = right[m, pl.ds(at, BLOCK), :]
                    out[begin + i] = jnp.where(row >= after, edge, out[begin + i])

                return _

            lax.fori_loop(0, count, fix, 0)


def overlay(layout, arrays, plan, offsets, packed, left, right):
    return pl.pallas_call(
        functools.partial(overlay_kernel, arrays),
        out_shape=[
            jax.ShapeDtypeStruct((layout.size(parts),) + packed[0].shape[1:], left.dtype)
            for parts in arrays
        ],
        in_specs=[smem()] * 2 + [vmem()] * (len(packed) + 2),
        out_specs=[vmem()] * len(arrays),
        compiler_params=pltpu.CompilerParams(vmem_limit_bytes=16 * MIB),
        cost_estimate=pl.CostEstimate(flops=1_000_000_000, bytes_accessed=4_000_000, transcendentals=0),
    )(plan, offsets, *packed, left, right)


def forward_kernel(layout, ranks, plan, *refs):
    n_data, n_tensor, per_pair = layout.n_data, layout.n_tensor, layout.per_pair
    outs = refs[-n_tensor:]
    for u in range(n_tensor):
        to = layout.target(0, u)
        swap = (plan[to, per_pair] == 0) & (plan[0, per_pair + 2] <= LATE)
        for k, rank in enumerate(ranks):
            for s in range(n_data):
                if rank == 0:

                    @pl.when(swap)
                    def _late(s=s, u=u):
                        outs[u][s] = refs[n_data + s][0]

                    @pl.when(jnp.logical_not(swap))
                    def _early(s=s, u=u):
                        outs[u][s] = refs[s][u]

                else:
                    outs[u][k * n_data + s] = refs[k * n_data + s][u]


def gather_forward(layout, ranks, plan, arrays):
    n_tensor = layout.n_tensor
    _, _, width = arrays[0].shape
    shape = jax.ShapeDtypeStruct((len(ranks) * layout.n_data, BLOCK, width), arrays[0].dtype)
    return pl.pallas_call(
        functools.partial(forward_kernel, layout, ranks),
        out_shape=[shape] * n_tensor,
        in_specs=[smem()] + [vmem()] * len(arrays),
        out_specs=[vmem()] * n_tensor,
        compiler_params=pltpu.CompilerParams(vmem_limit_bytes=12 * MIB),
        cost_estimate=pl.CostEstimate(flops=1_000_000_000, bytes_accessed=2_000_000, transcendentals=0),
    )(plan, *arrays)


def store_kernel(layout, ranks, direct, count, plan, *refs):
    n_data, n_tensor, per_pair = layout.n_data, layout.n_tensor, layout.per_pair
    incoming, probe = refs[:count], refs[count]
    stored, sketch, full, product, sems = refs[-5:]
    width = incoming[0].shape[-1]
    slots = len(ranks) * n_tensor
    step = min(4, slots)
    copies = []
    for begin in range(0, slots, step):
        for i in range(begin, begin + step):
            k, hop = i // n_tensor, i % n_tensor
            for s in range(n_data):
                if direct:
                    full[i, :, s * width : (s + 1) * width] = incoming[0][s, hop, k]
                else:
                    column = wrap(lax.axis_index("dp") - s + n_data, n_data)
                    columns = pl.ds(pl.multiple_of(column * width, width), width)
                    full[i, :, columns] = incoming[hop][k * n_data + s]
        span = pl.ds(begin, step)
        rows = full[span].reshape(step * BLOCK, n_data * width)
        dot = jnp.dot(rows, probe[...], preferred_element_type=jnp.float32)
        product[span] = dot.reshape(step, BLOCK, probe.shape[1])
        for i in range(begin, begin + step):
            k, u = i // n_tensor, i % n_tensor
            if direct:
                u = wrap(lax.axis_index("tensor") - u + n_tensor, n_tensor)
            slot = plan[u * per_pair + ranks[k], per_pair + 1]
            copies.append(pltpu.make_async_copy(full.at[i], stored.at[slot], sems.at[2 * i]))
            copies.append(pltpu.make_async_copy(product.at[i], sketch.at[slot], sems.at[2 * i + 1]))
            copies[-2].start()
            copies[-1].start()
    for copy in copies:
        copy.wait()


def store_ranks(layout, ranks, direct, plan, incoming, probe, previous):
    n_data, n_tensor, per_pair = layout.n_data, layout.n_tensor, layout.per_pair
    count = len(incoming)
    slots = len(ranks) * n_tensor
    columns = n_data * incoming[0].shape[-1]
    sketch_width = probe.shape[1]
    slot_count = n_tensor * per_pair
    out_shape = [
        jax.ShapeDtypeStruct((slot_count, BLOCK, columns), incoming[0].dtype),
        jax.ShapeDtypeStruct((slot_count, BLOCK, sketch_width), jnp.float32),
    ]
    held = [] if previous is None else list(previous)
    return pl.pallas_call(
        functools.partial(store_kernel, layout, ranks, direct, count),
        out_shape=out_shape,
        in_specs=[smem()] + [vmem()] * (count + 1) + [any_space() for _ in held],
        out_specs=[any_space(), any_space()],
        scratch_shapes=[
            pltpu.VMEM((slots, BLOCK, columns), incoming[0].dtype),
            pltpu.VMEM((slots, BLOCK, sketch_width), jnp.float32),
            pltpu.SemaphoreType.DMA((2 * slots,)),
        ],
        compiler_params=pltpu.CompilerParams(vmem_limit_bytes=(8 + 7 * slots // 8) * MIB),
        input_output_aliases={count + 2: 0, count + 3: 1} if held else {},
        cost_estimate=pl.CostEstimate(
            flops=2 * slots * BLOCK * columns * sketch_width,
            bytes_accessed=800_000 * slots,
            transcendentals=0,
        ),
    )(plan, *incoming, probe, *held)


def shards(embed_rows, head_rows, row_offsets, slot_table, probe):
    n_tensor = lax.axis_size("tensor")
    n_data = lax.axis_size("dp")
    quarter = R // 4
    devices = n_tensor * n_data
    per_pair = slot_table.shape[0] // devices // n_tensor
    layout = Layout(n_data, n_tensor, per_pair)

    lead_part, trail_part = cut_edges(row_offsets, embed_rows, head_rows, quarter)
    from_right = from_behind(lead_part, "tensor", -1)
    from_left = from_behind(trail_part, "tensor", 1)
    plan = make_plan(row_offsets, slot_table, n_data, n_tensor, per_pair)

    def move(block, s):
        if s == 0:
            return block
        return from_behind(block, "dp", s)

    def pack_all(arrays, limit):
        return pack(layout, arrays, plan, row_offsets, embed_rows, head_rows, limit)

    def overlay_all(arrays, packed):
        return overlay(layout, arrays, plan, row_offsets, packed, from_left, from_right)

    every_z = range(n_data)

    def send_z(group):
        return [move(group[s], s) for s in every_z]

    ranks = list(range(per_pair - layout.direct_ranks))
    rest = [layout.stage(rank) for rank in ranks[1:]] + [layout.direct()]
    if ranks:
        first = pack_all(layout.stage(0), 60)
        stages = {0: send_z(first)}
        rest = [layout.late()] + rest
    packed = pack_all([parts for group in rest for parts in group], 50)
    complete, at = [], 0
    for group in rest:
        complete.append(overlay_all(group, packed[at : at + len(group)]))
        at += len(group)
    if ranks:
        late = send_z(complete[0])
        for rank in ranks[1:]:
            stages[rank] = send_z(complete[rank])

        def resend(early):
            return send_z(overlay_all(layout.stage(0), first))

        crowded = plan[0, per_pair + 2] > LATE
        stages[0] = lax.cond(crowded, resend, lambda early: early, stages[0])
    direct = lax.all_to_all(
        complete[-1][0], ("dp", "tensor"), split_axis=0, concat_axis=0, tiled=True
    )
    direct = direct.reshape((n_data, n_tensor, layout.direct_ranks) + direct.shape[1:])
    outputs = None
    for rank in ranks:
        arrays = stages[rank] + (late if rank == 0 else [])
        gathered = gather_forward(layout, [rank], plan, arrays)
        forwarded = [gathered[0]]
        for u in range(1, n_tensor):
            forwarded.append(from_behind(gathered[u], "tensor", u))
        outputs = store_ranks(layout, [rank], False, plan, forwarded, probe, outputs)
    last = list(range(per_pair - layout.direct_ranks, per_pair))
    return tuple(store_ranks(layout, last, True, plan, [direct], probe, outputs))


def solution(mesh):
    return jax.shard_map(
        shards,
        mesh=mesh,
        in_specs=(P("tensor", "dp"), P("tensor", "dp"), P(), P(), P()),
        out_specs=(P(("dp", "tensor"), None, None), P(("dp", "tensor"), None, None)),
        check_vma=False,
    )
```

```python
import functools

import jax
import jax.numpy as jnp
from jax import lax
from jax.experimental import pallas as pl
from jax.experimental.pallas import tpu as pltpu
from jax.sharding import PartitionSpec as P


R = 8192
BLOCK = 128
LATE = 1
DIRECT = 2
ALIGN = 16
MIB = 1 << 20


def from_behind(block, axis, distance):
    devices = range(lax.axis_size(axis))
    route = [((i - distance) % len(devices), i) for i in devices]
    return lax.ppermute(block, axis, route)


def any_space():
    return pl.BlockSpec(memory_space=pl.ANY)


def in_hbm():
    return pl.BlockSpec(memory_space=pltpu.HBM)


def smem():
    return pl.BlockSpec(memory_space=pltpu.SMEM)


def vmem():
    return pl.BlockSpec(memory_space=pltpu.VMEM)


def my_span(offsets, m):
    t = lax.axis_index("tensor")
    return offsets[m, t] - t * R, offsets[m, t + 1] - t * R


def edges_kernel(offsets, embed, head, lead_out, trail_out, rows, wide, sems):
    quarter = lead_out.shape[1]
    raws = [embed, head]
    copies = []
    for m in range(2):
        first = (R - my_span(offsets, m)[0]) & -ALIGN
        window = pl.ds(pl.multiple_of(first, ALIGN), quarter + ALIGN)
        lead = pltpu.make_async_copy(
            raws[m].at[pl.ds(0, quarter)], rows.at[2 * m, pl.ds(0, quarter)], sems.at[2 * m]
        )
        trail = pltpu.make_async_copy(raws[m].at[window], rows.at[2 * m + 1], sems.at[2 * m + 1])
        lead.start()
        trail.start()
        copies.append((lead, trail))
    blocks = quarter // BLOCK
    for m in range(2):
        lead, trail = copies[m]
        before, after = my_span(offsets, m)
        lead.wait()
        count = jnp.clip(-before, 0, quarter)
        used = (count + BLOCK - 1) >> log2(BLOCK)

        def widen_lead(i, _):
            at = pl.multiple_of(i * BLOCK, BLOCK)
            wide[pl.ds(quarter + at, BLOCK), :] = rows[2 * m, pl.ds(at, BLOCK), :].astype(jnp.float32)
            return _

        lax.fori_loop(0, used, widen_lead, 0)

        def put_lead(i, _):
            at = pl.multiple_of(i * BLOCK, BLOCK)
            lead_out[m, pl.ds(at, BLOCK), :] = wide[pl.ds(count + at, BLOCK), :].astype(jnp.bfloat16)
            return _

        lax.fori_loop(blocks - used, blocks, put_lead, 0)
        trail.wait()
        shift = (R - before) & (ALIGN - 1)
        used = (jnp.clip(after - R, 0, quarter) + BLOCK - 1) >> log2(BLOCK)

        def widen_trail(i, _):
            at = pl.multiple_of(i * BLOCK, BLOCK)
            wide[pl.ds(at, BLOCK), :] = rows[2 * m + 1, pl.ds(at, BLOCK), :].astype(jnp.float32)
            return _

        lax.fori_loop(0, jnp.minimum(used + 1, blocks), widen_trail, 0)

        @pl.when(used == blocks)
        def _last():
            wide[pl.ds(quarter, ALIGN), :] = rows[2 * m + 1, pl.ds(quarter, ALIGN), :].astype(jnp.float32)

        def put_trail(i, _):
            at = pl.multiple_of(i * BLOCK, BLOCK)
            trail_out[m, pl.ds(at, BLOCK), :] = wide[pl.ds(shift + at, BLOCK), :].astype(jnp.bfloat16)
            return _

        lax.fori_loop(0, used, put_trail, 0)


def cut_edges(offsets, embed, head, quarter):
    width = embed.shape[1]
    shape = jax.ShapeDtypeStruct((2, quarter, width), embed.dtype)
    return pl.pallas_call(
        edges_kernel,
        out_shape=(shape, shape),
        in_specs=[smem(), in_hbm(), in_hbm()],
        out_specs=[vmem()] * 2,
        scratch_shapes=[
            pltpu.VMEM((4, quarter + ALIGN, width), embed.dtype),
            pltpu.VMEM((2 * quarter, width), jnp.float32),
            pltpu.SemaphoreType.DMA((4,)),
        ],
        compiler_params=pltpu.CompilerParams(vmem_limit_bytes=61 * MIB),
    )(offsets, embed, head)


def log2(size):
    assert size & (size - 1) == 0
    return size.bit_length() - 1


def wrap(index, size):
    return index & (size - 1)


def target(s, u, n_data, n_tensor):
    z = wrap(lax.axis_index("dp") + s, n_data)
    t = wrap(lax.axis_index("tensor") + u, n_tensor)
    return z * n_tensor + t


def split_block(block):
    bits = log2(R // BLOCK)
    return block >> bits, (block & (R // BLOCK - 1)) * BLOCK


def plan_kernel(n_data, n_tensor, per_pair, offsets, slots, plan):
    devices, count = slots.shape
    per_rank = R // BLOCK
    total = per_rank * n_tensor
    slot = slots[...]
    matrix = slot >> log2(total)
    rest = slot & (total - 1)
    source = rest >> log2(per_rank)
    k = rest & (per_rank - 1)
    local = jnp.zeros_like(slot)
    for m in range(2):
        for t in range(n_tensor):
            begin = offsets[m, t] - t * R
            end = offsets[m, t + 1] - t * R
            inside = (k * BLOCK >= begin) & (k * BLOCK + BLOCK <= end)
            here = (source == t) & (matrix == m)
            local = jnp.where(here & inside, 1, local)
    column = lax.broadcasted_iota(jnp.int32, slot.shape, 1)
    lowest = source * (2 * count)
    key = lowest + (1 - local) * count + column
    rank = jnp.zeros_like(slot)
    for j in range(count):
        other = key[:, j : j + 1]
        rank += jnp.where((other >= lowest) & (other < key), 1, 0)
    my_t = lax.axis_index("tensor")
    me = lax.axis_index("dp") * n_tensor + my_t
    lane = lax.broadcasted_iota(jnp.int32, plan.shape, 1)
    row = lax.broadcasted_iota(jnp.int32, slot.shape, 0)
    out = jnp.zeros(plan.shape, jnp.int32)
    block = matrix * per_rank + k
    for r in range(per_pair):
        mine = (source == my_t) & (rank == r)
        picked = jnp.sum(jnp.where(mine, block, 0), axis=1, keepdims=True)
        out = jnp.where(lane == r, picked, out)
        if r == 0:
            flag = jnp.sum(jnp.where(mine, local, 0), axis=1, keepdims=True)
            out = jnp.where(lane == per_pair, flag, out)
    hops = (my_t - source) & (n_tensor - 1)
    order = jnp.where(row == me, hops * per_pair + rank, 0)
    order = jnp.sum(order, axis=0, keepdims=True)
    found = jnp.where(order == row, column, 0)
    out = jnp.where(lane == per_pair + 1, jnp.sum(found, axis=1, keepdims=True), out)
    empty = jnp.zeros(plan.shape, jnp.int32)
    for t in range(n_tensor):
        has = jnp.max(jnp.where(source == t, local, 0), axis=1, keepdims=True)
        empty = jnp.where(lane == t, 1 - has, empty)
    worst = jnp.zeros((1, 1), jnp.int32)
    for z in range(n_data):
        layer = jnp.sum(empty[z * n_tensor : (z + 1) * n_tensor], axis=0, keepdims=True)
        worst = jnp.maximum(worst, jnp.max(layer, axis=1, keepdims=True))
    plan[...] = jnp.where(lane == per_pair + 2, worst, out)


def make_plan(offsets, slot_table, n_data, n_tensor, per_pair):
    devices = n_data * n_tensor
    return pl.pallas_call(
        functools.partial(plan_kernel, n_data, n_tensor, per_pair),
        out_shape=jax.ShapeDtypeStruct((devices, 128), jnp.int32),
        in_specs=[smem(), vmem()],
        out_specs=vmem(),
        compiler_params=pltpu.CompilerParams(vmem_limit_bytes=4 * MIB),
    )(offsets, slot_table.reshape(devices, -1))


class Layout:
    def __init__(self, n_data, n_tensor, per_pair):
        self.n_data, self.n_tensor, self.per_pair = n_data, n_tensor, per_pair
        self.staged = per_pair > DIRECT + 1
        self.direct_ranks = DIRECT if self.staged else per_pair

    def target(self, s, u):
        return target(s, u, self.n_data, self.n_tensor)

    def along_z(self, s, rank):
        return (0, self.n_tensor, lambda plan, i: plan[self.target(s, i), rank])

    def late_block(self, plan, s):
        chosen = self.target(s, 0)
        for u in reversed(range(self.n_tensor)):
            to = self.target(s, u)
            chosen = jnp.where(plan[to, self.per_pair] == 0, to, chosen)
        return plan[chosen, 0]

    def late(self):
        return [
            [(0, LATE, lambda plan, i, s=s: self.late_block(plan, s))] for s in range(self.n_data)
        ]

    def stage(self, rank):
        return [[self.along_z(s, rank)] for s in range(self.n_data)]

    def direct(self):
        count, first = self.direct_ranks, self.per_pair - self.direct_ranks
        bits = log2(count)
        which = lambda plan, i: plan[i >> bits, first + (i & (count - 1))]
        return [[(0, self.n_data * self.n_tensor * count, which)]]

    def size(self, parts):
        return sum(part[1] for part in parts)


def pack_kernel(arrays, plan, offsets, embed, head, *refs):
    outs, (windows, wide, sems) = refs[: len(arrays)], refs[len(arrays) :]
    height = embed.shape[0]

    t = lax.axis_index("tensor")
    begins = [offsets[m, t] - t * R for m in range(2)]

    def where_from(block):
        m, row = split_block(block)
        start = row - jnp.where(m == 0, begins[0], begins[1])
        start = jnp.minimum(jnp.maximum(start + BLOCK, 0), height - ALIGN)
        first = jnp.maximum((start & -ALIGN) - BLOCK, 0)
        return m, start - BLOCK, pl.multiple_of(first, ALIGN)

    at = 0
    for parts in arrays:
        for begin, count, which in parts:

            def fetch(i, _, at=at, which=which):
                m, _start, first = where_from(which(plan, i))
                for k, raw in enumerate([embed, head]):

                    @pl.when(m == k)
                    def _fetch(raw=raw):
                        pltpu.make_async_copy(
                            raw.at[pl.ds(first, BLOCK + ALIGN)], windows.at[at + i], sems.at[at + i]
                        ).start()

                return _

            lax.fori_loop(0, count, fetch, 0)
            at += count
    at = 0
    for parts, out in zip(arrays, outs):
        for begin, count, which in parts:

            def shift(i, _, at=at, which=which, out=out, begin=begin):
                m, start, first = where_from(which(plan, i))
                pltpu.make_async_copy(
                    embed.at[pl.ds(0, BLOCK + ALIGN)], windows.at[at + i], sems.at[at + i]
                ).wait()
                slot = i & 1
                wide[slot, pl.ds(BLOCK, BLOCK + ALIGN), :] = windows[at + i].astype(jnp.float32)
                moved = wide[slot, pl.ds(BLOCK + start - first, BLOCK), :]
                out[begin + i] = moved.astype(jnp.bfloat16)
                return _

            lax.fori_loop(0, count, shift, 0)
            at += count


def pack(layout, arrays, plan, offsets, embed, head, limit):
    width = embed.shape[1]
    total = sum(layout.size(parts) for parts in arrays)
    return pl.pallas_call(
        functools.partial(pack_kernel, arrays),
        out_shape=[
            jax.ShapeDtypeStruct((layout.size(parts), BLOCK, width), embed.dtype) for parts in arrays
        ],
        in_specs=[smem(), smem(), in_hbm(), in_hbm()],
        out_specs=[vmem()] * len(arrays),
        scratch_shapes=[
            pltpu.VMEM((total, BLOCK + ALIGN, width), embed.dtype),
            pltpu.VMEM((2, 2 * BLOCK + ALIGN, width), jnp.float32),
            pltpu.SemaphoreType.DMA((total,)),
        ],
        compiler_params=pltpu.CompilerParams(vmem_limit_bytes=limit * MIB),
        cost_estimate=pl.CostEstimate(flops=total * 30_000_000, bytes_accessed=total * 70_000, transcendentals=0),
    )(plan, offsets, embed, head)


def overlay_kernel(arrays, plan, offsets, *refs):
    packed, left, right, outs = refs[: len(arrays)], refs[-len(arrays) - 2], refs[-len(arrays) - 1], refs[-len(arrays) :]
    quarter = left.shape[1]
    t = lax.axis_index("tensor")
    begins = [offsets[m, t] - t * R for m in range(2)]
    ends = [offsets[m, t + 1] - t * R for m in range(2)]
    for parts, source, out in zip(arrays, packed, outs):
        out[...] = source[...]
        for begin, count, which in parts:

            def fix(i, _, begin=begin, which=which, out=out):
                m, first = split_block(which(plan, i))
                before = jnp.where(m == 0, begins[0], begins[1])
                after = jnp.where(m == 0, ends[0], ends[1])

                @pl.when(first < before)
                def _left():
                    row = first + lax.broadcasted_iota(jnp.int32, (BLOCK, 1), 0)
                    edge = left[m, pl.ds(pl.multiple_of(first, BLOCK), BLOCK), :]
                    out[begin + i] = jnp.where(row < before, edge, out[begin + i])

                @pl.when(first + BLOCK > after)
                def _right():
                    row = first + lax.broadcasted_iota(jnp.int32, (BLOCK, 1), 0)
                    at = pl.multiple_of(first - (R - quarter), BLOCK)
                    edge = right[m, pl.ds(at, BLOCK), :]
                    out[begin + i] = jnp.where(row >= after, edge, out[begin + i])

                return _

            lax.fori_loop(0, count, fix, 0)


def overlay(layout, arrays, plan, offsets, packed, left, right):
    return pl.pallas_call(
        functools.partial(overlay_kernel, arrays),
        out_shape=[
            jax.ShapeDtypeStruct((layout.size(parts),) + packed[0].shape[1:], left.dtype)
            for parts in arrays
        ],
        in_specs=[smem()] * 2 + [vmem()] * (len(packed) + 2),
        out_specs=[vmem()] * len(arrays),
        compiler_params=pltpu.CompilerParams(vmem_limit_bytes=16 * MIB),
        cost_estimate=pl.CostEstimate(flops=1_000_000_000, bytes_accessed=4_000_000, transcendentals=0),
    )(plan, offsets, *packed, left, right)


def forward_kernel(layout, ranks, plan, *refs):
    n_data, n_tensor, per_pair = layout.n_data, layout.n_tensor, layout.per_pair
    outs = refs[-n_tensor:]
    for u in range(n_tensor):
        to = layout.target(0, u)
        swap = (plan[to, per_pair] == 0) & (plan[0, per_pair + 2] <= LATE)
        for k, rank in enumerate(ranks):
            for s in range(n_data):
                if rank == 0:

                    @pl.when(swap)
                    def _late(s=s, u=u):
                        outs[u][s] = refs[n_data + s][0]

                    @pl.when(jnp.logical_not(swap))
                    def _early(s=s, u=u):
                        outs[u][s] = refs[s][u]

                else:
                    outs[u][k * n_data + s] = refs[k * n_data + s][u]


def gather_forward(layout, ranks, plan, arrays):
    n_tensor = layout.n_tensor
    _, _, width = arrays[0].shape
    shape = jax.ShapeDtypeStruct((len(ranks) * layout.n_data, BLOCK, width), arrays[0].dtype)
    return pl.pallas_call(
        functools.partial(forward_kernel, layout, ranks),
        out_shape=[shape] * n_tensor,
        in_specs=[smem()] + [vmem()] * len(arrays),
        out_specs=[vmem()] * n_tensor,
        compiler_params=pltpu.CompilerParams(vmem_limit_bytes=12 * MIB),
        cost_estimate=pl.CostEstimate(flops=1_000_000_000, bytes_accessed=2_000_000, transcendentals=0),
    )(plan, *arrays)


def store_kernel(layout, ranks, direct, count, plan, *refs):
    n_data, n_tensor, per_pair = layout.n_data, layout.n_tensor, layout.per_pair
    incoming, probe = refs[:count], refs[count]
    stored, sketch, full, product, sems = refs[-5:]
    width = incoming[0].shape[-1]
    slots = len(ranks) * n_tensor
    copies = []
    begin = 0
    while begin < slots:
        step = min(max(begin, 1), 4, slots - begin)
        for i in range(begin, begin + step):
            k, hop = i // n_tensor, i % n_tensor
            for s in range(n_data):
                if direct:
                    full[i, :, s * width : (s + 1) * width] = incoming[0][s, hop, k]
                else:
                    column = wrap(lax.axis_index("dp") - s + n_data, n_data)
                    columns = pl.ds(pl.multiple_of(column * width, width), width)
                    full[i, :, columns] = incoming[hop][k * n_data + s]
        span = pl.ds(begin, step)
        rows = full[span].reshape(step * BLOCK, n_data * width)
        dot = jnp.dot(rows, probe[...], preferred_element_type=jnp.float32)
        product[span] = dot.reshape(step, BLOCK, probe.shape[1])
        for i in range(begin, begin + step):
            k, u = i // n_tensor, i % n_tensor
            if direct:
                u = wrap(lax.axis_index("tensor") - u + n_tensor, n_tensor)
            slot = plan[u * per_pair + ranks[k], per_pair + 1]
            copies.append(pltpu.make_async_copy(full.at[i], stored.at[slot], sems.at[2 * i]))
            copies.append(pltpu.make_async_copy(product.at[i], sketch.at[slot], sems.at[2 * i + 1]))
            copies[-2].start()
            copies[-1].start()
        begin += step
    for copy in copies:
        copy.wait()


def store_ranks(layout, ranks, direct, plan, incoming, probe, previous):
    n_data, n_tensor, per_pair = layout.n_data, layout.n_tensor, layout.per_pair
    count = len(incoming)
    slots = len(ranks) * n_tensor
    columns = n_data * incoming[0].shape[-1]
    sketch_width = probe.shape[1]
    slot_count = n_tensor * per_pair
    out_shape = [
        jax.ShapeDtypeStruct((slot_count, BLOCK, columns), incoming[0].dtype),
        jax.ShapeDtypeStruct((slot_count, BLOCK, sketch_width), jnp.float32),
    ]
    held = [] if previous is None else list(previous)
    return pl.pallas_call(
        functools.partial(store_kernel, layout, ranks, direct, count),
        out_shape=out_shape,
        in_specs=[smem()] + [vmem()] * (count + 1) + [any_space() for _ in held],
        out_specs=[any_space(), any_space()],
        scratch_shapes=[
            pltpu.VMEM((slots, BLOCK, columns), incoming[0].dtype),
            pltpu.VMEM((slots, BLOCK, sketch_width), jnp.float32),
            pltpu.SemaphoreType.DMA((2 * slots,)),
        ],
        compiler_params=pltpu.CompilerParams(vmem_limit_bytes=(8 + 7 * slots // 8) * MIB),
        input_output_aliases={count + 2: 0, count + 3: 1} if held else {},
        cost_estimate=pl.CostEstimate(
            flops=2 * slots * BLOCK * columns * sketch_width,
            bytes_accessed=800_000 * slots,
            transcendentals=0,
        ),
    )(plan, *incoming, probe, *held)


def shards(embed_rows, head_rows, row_offsets, slot_table, probe):
    n_tensor = lax.axis_size("tensor")
    n_data = lax.axis_size("dp")
    quarter = R // 4
    devices = n_tensor * n_data
    per_pair = slot_table.shape[0] // devices // n_tensor
    layout = Layout(n_data, n_tensor, per_pair)

    lead_part, trail_part = cut_edges(row_offsets, embed_rows, head_rows, quarter)
    from_right = from_behind(lead_part, "tensor", -1)
    from_left = from_behind(trail_part, "tensor", 1)
    plan = make_plan(row_offsets, slot_table, n_data, n_tensor, per_pair)

    def move(block, s):
        if s == 0:
            return block
        return from_behind(block, "dp", s)

    def pack_all(arrays, limit):
        return pack(layout, arrays, plan, row_offsets, embed_rows, head_rows, limit)

    def overlay_all(arrays, packed):
        return overlay(layout, arrays, plan, row_offsets, packed, from_left, from_right)

    every_z = range(n_data)

    def send_z(group):
        return [move(group[s], s) for s in every_z]

    ranks = list(range(per_pair - layout.direct_ranks))
    rest = [layout.stage(rank) for rank in ranks[1:]] + [layout.direct()]
    if ranks:
        first = pack_all(layout.stage(0), 60)
        stages = {0: send_z(first)}
        rest = [layout.late() + rest[0]] + rest[1:]
    packed = pack_all([parts for group in rest for parts in group], 50)
    complete, at = [], 0
    for group in rest:
        complete.append(overlay_all(group, packed[at : at + len(group)]))
        at += len(group)
    if ranks:
        late = send_z(complete[0][:n_data])
        for rank in ranks[1:]:
            stages[rank] = send_z(complete[0][n_data * rank :])

        def resend(early):
            return send_z(overlay_all(layout.stage(0), first))

        crowded = plan[0, per_pair + 2] > LATE
        stages[0] = lax.cond(crowded, resend, lambda early: early, stages[0])
    direct = lax.all_to_all(
        complete[-1][0], ("dp", "tensor"), split_axis=0, concat_axis=0, tiled=True
    )
    direct = direct.reshape((n_data, n_tensor, layout.direct_ranks) + direct.shape[1:])
    outputs = None
    for rank in ranks:
        arrays = stages[rank] + (late if rank == 0 else [])
        gathered = gather_forward(layout, [rank], plan, arrays)
        forwarded = [gathered[0]]
        for u in range(1, n_tensor):
            forwarded.append(from_behind(gathered[u], "tensor", u))
        outputs = store_ranks(layout, [rank], False, plan, forwarded, probe, outputs)
    last = list(range(per_pair - layout.direct_ranks, per_pair))
    return tuple(store_ranks(layout, last, True, plan, [direct], probe, outputs))


def solution(mesh):
    return jax.shard_map(
        shards,
        mesh=mesh,
        in_specs=(P("tensor", "dp"), P("tensor", "dp"), P(), P(), P()),
        out_specs=(P(("dp", "tensor"), None, None), P(("dp", "tensor"), None, None)),
        check_vma=False,
    )
```

```python
import functools

import jax
import jax.numpy as jnp
from jax import lax
from jax.experimental import pallas as pl
from jax.experimental.pallas import tpu as pltpu
from jax.sharding import PartitionSpec as P


R = 8192
BLOCK = 128
LATE = 1
DIRECT = 2
ALIGN = 16
MIB = 1 << 20


def from_behind(block, axis, distance):
    devices = range(lax.axis_size(axis))
    route = [((i - distance) % len(devices), i) for i in devices]
    return lax.ppermute(block, axis, route)


def any_space():
    return pl.BlockSpec(memory_space=pl.ANY)


def in_hbm():
    return pl.BlockSpec(memory_space=pltpu.HBM)


def smem():
    return pl.BlockSpec(memory_space=pltpu.SMEM)


def vmem():
    return pl.BlockSpec(memory_space=pltpu.VMEM)


def my_span(offsets, m):
    t = lax.axis_index("tensor")
    return offsets[m, t] - t * R, offsets[m, t + 1] - t * R


def edges_kernel(offsets, embed, head, lead_out, trail_out, lead_in, trail_in, sems, out_sems):
    quarter = lead_out.shape[1]
    copies = []
    writes = []
    for m, raw in enumerate([embed, head]):
        first = (R - my_span(offsets, m)[0]) & -ALIGN
        window = pl.ds(pl.multiple_of(first, ALIGN), quarter + ALIGN)
        copies.append(
            pltpu.make_async_copy(raw.at[pl.ds(0, quarter)], lead_in.at[m], sems.at[2 * m])
        )
        copies.append(pltpu.make_async_copy(raw.at[window], trail_in.at[m], sems.at[2 * m + 1]))
        writes.append(pltpu.make_async_copy(lead_in.at[m], lead_out.at[m], out_sems.at[2 * m]))
        writes.append(pltpu.make_async_copy(trail_in.at[m], trail_out.at[m], out_sems.at[2 * m + 1]))
    for copy in copies:
        copy.start()
    for copy, write in zip(copies, writes):
        copy.wait()
        write.start()
    for write in writes:
        write.wait()


def cut_edges(offsets, embed, head, quarter):
    width = embed.shape[1]
    return pl.pallas_call(
        edges_kernel,
        out_shape=[
            jax.ShapeDtypeStruct((2, rows, width), embed.dtype) for rows in (quarter, quarter + ALIGN)
        ],
        in_specs=[smem(), in_hbm(), in_hbm()],
        out_specs=[in_hbm()] * 2,
        scratch_shapes=[
            pltpu.VMEM((2, quarter, width), embed.dtype),
            pltpu.VMEM((2, quarter + ALIGN, width), embed.dtype),
            pltpu.SemaphoreType.DMA((4,)),
            pltpu.SemaphoreType.DMA((4,)),
        ],
        compiler_params=pltpu.CompilerParams(vmem_limit_bytes=61 * MIB),
    )(offsets, embed, head)


def log2(size):
    assert size & (size - 1) == 0
    return size.bit_length() - 1


def wrap(index, size):
    return index & (size - 1)


def target(s, u, n_data, n_tensor):
    z = wrap(lax.axis_index("dp") + s, n_data)
    t = wrap(lax.axis_index("tensor") + u, n_tensor)
    return z * n_tensor + t


def split_block(block):
    bits = log2(R // BLOCK)
    return block >> bits, (block & (R // BLOCK - 1)) * BLOCK


def plan_kernel(n_data, n_tensor, per_pair, offsets, slots, plan):
    devices, count = slots.shape
    per_rank = R // BLOCK
    total = per_rank * n_tensor
    slot = slots[...]
    matrix = slot >> log2(total)
    rest = slot & (total - 1)
    source = rest >> log2(per_rank)
    k = rest & (per_rank - 1)
    local = jnp.zeros_like(slot)
    for m in range(2):
        for t in range(n_tensor):
            begin = offsets[m, t] - t * R
            end = offsets[m, t + 1] - t * R
            inside = (k * BLOCK >= begin) & (k * BLOCK + BLOCK <= end)
            here = (source == t) & (matrix == m)
            local = jnp.where(here & inside, 1, local)
    column = lax.broadcasted_iota(jnp.int32, slot.shape, 1)
    lowest = source * (2 * count)
    key = lowest + (1 - local) * count + column
    rank = jnp.zeros_like(slot)
    for j in range(count):
        other = key[:, j : j + 1]
        rank += jnp.where((other >= lowest) & (other < key), 1, 0)
    my_t = lax.axis_index("tensor")
    me = lax.axis_index("dp") * n_tensor + my_t
    lane = lax.broadcasted_iota(jnp.int32, plan.shape, 1)
    row = lax.broadcasted_iota(jnp.int32, slot.shape, 0)
    out = jnp.zeros(plan.shape, jnp.int32)
    block = matrix * per_rank + k
    for r in range(per_pair):
        mine = (source == my_t) & (rank == r)
        picked = jnp.sum(jnp.where(mine, block, 0), axis=1, keepdims=True)
        out = jnp.where(lane == r, picked, out)
        if r == 0:
            flag = jnp.sum(jnp.where(mine, local, 0), axis=1, keepdims=True)
            out = jnp.where(lane == per_pair, flag, out)
    hops = (my_t - source) & (n_tensor - 1)
    order = jnp.where(row == me, hops * per_pair + rank, 0)
    order = jnp.sum(order, axis=0, keepdims=True)
    found = jnp.where(order == row, column, 0)
    out = jnp.where(lane == per_pair + 1, jnp.sum(found, axis=1, keepdims=True), out)
    empty = jnp.zeros(plan.shape, jnp.int32)
    for t in range(n_tensor):
        has = jnp.max(jnp.where(source == t, local, 0), axis=1, keepdims=True)
        empty = jnp.where(lane == t, 1 - has, empty)
    worst = jnp.zeros((1, 1), jnp.int32)
    for z in range(n_data):
        layer = jnp.sum(empty[z * n_tensor : (z + 1) * n_tensor], axis=0, keepdims=True)
        worst = jnp.maximum(worst, jnp.max(layer, axis=1, keepdims=True))
    plan[...] = jnp.where(lane == per_pair + 2, worst, out)


def make_plan(offsets, slot_table, n_data, n_tensor, per_pair):
    devices = n_data * n_tensor
    return pl.pallas_call(
        functools.partial(plan_kernel, n_data, n_tensor, per_pair),
        out_shape=jax.ShapeDtypeStruct((devices, 128), jnp.int32),
        in_specs=[smem(), vmem()],
        out_specs=vmem(),
        compiler_params=pltpu.CompilerParams(vmem_limit_bytes=4 * MIB),
    )(offsets, slot_table.reshape(devices, -1))


class Layout:
    def __init__(self, n_data, n_tensor, per_pair):
        self.n_data, self.n_tensor, self.per_pair = n_data, n_tensor, per_pair
        self.staged = per_pair > DIRECT + 1
        self.direct_ranks = DIRECT if self.staged else per_pair

    def target(self, s, u):
        return target(s, u, self.n_data, self.n_tensor)

    def along_z(self, s, rank):
        return (0, self.n_tensor, lambda plan, i: plan[self.target(s, i), rank])

    def late_block(self, plan, s):
        chosen = self.target(s, 0)
        for u in reversed(range(self.n_tensor)):
            to = self.target(s, u)
            chosen = jnp.where(plan[to, self.per_pair] == 0, to, chosen)
        return plan[chosen, 0]

    def late(self):
        return [
            [(0, LATE, lambda plan, i, s=s: self.late_block(plan, s))] for s in range(self.n_data)
        ]

    def stage(self, rank):
        return [[self.along_z(s, rank)] for s in range(self.n_data)]

    def direct(self):
        count, first = self.direct_ranks, self.per_pair - self.direct_ranks
        bits = log2(count)
        which = lambda plan, i: plan[i >> bits, first + (i & (count - 1))]
        return [[(0, self.n_data * self.n_tensor * count, which)]]

    def size(self, parts):
        return sum(part[1] for part in parts)


def pack_kernel(arrays, plan, offsets, embed, head, *refs):
    outs, (windows, wide, sems) = refs[: len(arrays)], refs[len(arrays) :]
    height = embed.shape[0]

    t = lax.axis_index("tensor")
    begins = [offsets[m, t] - t * R for m in range(2)]

    def where_from(block):
        m, row = split_block(block)
        start = row - jnp.where(m == 0, begins[0], begins[1])
        start = jnp.minimum(jnp.maximum(start + BLOCK, 0), height - ALIGN)
        first = jnp.maximum((start & -ALIGN) - BLOCK, 0)
        return m, start - BLOCK, pl.multiple_of(first, ALIGN)

    at = 0
    for parts in arrays:
        for begin, count, which in parts:

            def fetch(i, _, at=at, which=which):
                m, _start, first = where_from(which(plan, i))
                for k, raw in enumerate([embed, head]):

                    @pl.when(m == k)
                    def _fetch(raw=raw):
                        pltpu.make_async_copy(
                            raw.at[pl.ds(first, BLOCK + ALIGN)], windows.at[at + i], sems.at[at + i]
                        ).start()

                return _

            lax.fori_loop(0, count, fetch, 0)
            at += count
    at = 0
    for parts, out in zip(arrays, outs):
        for begin, count, which in parts:

            def shift(i, _, at=at, which=which, out=out, begin=begin):
                m, start, first = where_from(which(plan, i))
                pltpu.make_async_copy(
                    embed.at[pl.ds(0, BLOCK + ALIGN)], windows.at[at + i], sems.at[at + i]
                ).wait()
                slot = i & 1
                wide[slot, pl.ds(BLOCK, BLOCK + ALIGN), :] = windows[at + i].astype(jnp.float32)
                moved = wide[slot, pl.ds(BLOCK + start - first, BLOCK), :]
                out[begin + i] = moved.astype(jnp.bfloat16)
                return _

            lax.fori_loop(0, count, shift, 0)
            at += count


def pack(layout, arrays, plan, offsets, embed, head, limit):
    width = embed.shape[1]
    total = sum(layout.size(parts) for parts in arrays)
    return pl.pallas_call(
        functools.partial(pack_kernel, arrays),
        out_shape=[
            jax.ShapeDtypeStruct((layout.size(parts), BLOCK, width), embed.dtype) for parts in arrays
        ],
        in_specs=[smem(), smem(), in_hbm(), in_hbm()],
        out_specs=[vmem()] * len(arrays),
        scratch_shapes=[
            pltpu.VMEM((total, BLOCK + ALIGN, width), embed.dtype),
            pltpu.VMEM((2, 2 * BLOCK + ALIGN, width), jnp.float32),
            pltpu.SemaphoreType.DMA((total,)),
        ],
        compiler_params=pltpu.CompilerParams(vmem_limit_bytes=limit * MIB),
        cost_estimate=pl.CostEstimate(flops=total * 30_000_000, bytes_accessed=total * 70_000, transcendentals=0),
    )(plan, offsets, embed, head)


def overlay_kernel(arrays, n_tensor, plan, offsets, *refs):
    count = len(arrays)
    packed, left, right, outs, wide = refs[:count], refs[count], refs[count + 1], refs[-count - 1 : -1], refs[-1]
    quarter = right.shape[1]
    t = lax.axis_index("tensor")
    begins = [offsets[m, t] - t * R for m in range(2)]
    ends = [offsets[m, t + 1] - t * R for m in range(2)]
    behind = wrap(t + n_tensor - 1, n_tensor)
    shifts = [(R - offsets[m, behind] + behind * R) & (ALIGN - 1) for m in range(2)]
    for parts, source, out in zip(arrays, packed, outs):
        out[...] = source[...]
        for begin, blocks, which in parts:

            def fix(i, _, begin=begin, which=which, out=out):
                m, first = split_block(which(plan, i))
                before = jnp.where(m == 0, begins[0], begins[1])
                after = jnp.where(m == 0, ends[0], ends[1])

                @pl.when((first < before) | (first + BLOCK > after))
                def _edge():
                    @pl.when(first < before)
                    def _left():
                        row = first + lax.broadcasted_iota(jnp.int32, (BLOCK, 1), 0)
                        window = pl.ds(pl.multiple_of(first, BLOCK), BLOCK + ALIGN)
                        wide[pl.ds(0, BLOCK + ALIGN), :] = left[m, window, :].astype(jnp.float32)
                        shift = jnp.where(m == 0, shifts[0], shifts[1])
                        edge = wide[pl.ds(shift, BLOCK), :].astype(out.dtype)
                        out[begin + i] = jnp.where(row < before, edge, out[begin + i])

                    @pl.when(first + BLOCK > after)
                    def _right():
                        row = first + lax.broadcasted_iota(jnp.int32, (BLOCK, 1), 0)
                        start = first - after
                        at = jnp.clip(start & -ALIGN, 0, quarter - BLOCK - ALIGN)
                        window = pl.ds(pl.multiple_of(at, ALIGN), BLOCK + ALIGN)
                        wide[pl.ds(BLOCK, BLOCK + ALIGN), :] = right[m, window, :].astype(jnp.float32)
                        edge = wide[pl.ds(BLOCK + start - at, BLOCK), :].astype(out.dtype)
                        out[begin + i] = jnp.where(row >= after, edge, out[begin + i])

                return _

            lax.fori_loop(0, blocks, fix, 0)


def overlay(layout, arrays, plan, offsets, packed, left, right):
    return pl.pallas_call(
        functools.partial(overlay_kernel, arrays, layout.n_tensor),
        out_shape=[
            jax.ShapeDtypeStruct((layout.size(parts),) + packed[0].shape[1:], left.dtype)
            for parts in arrays
        ],
        in_specs=[smem()] * 2 + [vmem()] * (len(packed) + 2),
        out_specs=[vmem()] * len(arrays),
        scratch_shapes=[pltpu.VMEM((2 * BLOCK + ALIGN, packed[0].shape[2]), jnp.float32)],
        compiler_params=pltpu.CompilerParams(vmem_limit_bytes=16 * MIB),
        cost_estimate=pl.CostEstimate(flops=1_000_000_000, bytes_accessed=4_000_000, transcendentals=0),
    )(plan, offsets, *packed, left, right)


def forward_kernel(layout, ranks, plan, *refs):
    n_data, n_tensor, per_pair = layout.n_data, layout.n_tensor, layout.per_pair
    outs = refs[-n_tensor:]
    for u in range(n_tensor):
        to = layout.target(0, u)
        swap = (plan[to, per_pair] == 0) & (plan[0, per_pair + 2] <= LATE)
        for k, rank in enumerate(ranks):
            for s in range(n_data):
                if rank == 0:

                    @pl.when(swap)
                    def _late(s=s, u=u):
                        outs[u][s] = refs[n_data + s][0]

                    @pl.when(jnp.logical_not(swap))
                    def _early(s=s, u=u):
                        outs[u][s] = refs[s][u]

                else:
                    outs[u][k * n_data + s] = refs[k * n_data + s][u]


def gather_forward(layout, ranks, plan, arrays):
    n_tensor = layout.n_tensor
    _, _, width = arrays[0].shape
    shape = jax.ShapeDtypeStruct((len(ranks) * layout.n_data, BLOCK, width), arrays[0].dtype)
    return pl.pallas_call(
        functools.partial(forward_kernel, layout, ranks),
        out_shape=[shape] * n_tensor,
        in_specs=[smem()] + [vmem()] * len(arrays),
        out_specs=[vmem()] * n_tensor,
        compiler_params=pltpu.CompilerParams(vmem_limit_bytes=12 * MIB),
        cost_estimate=pl.CostEstimate(flops=1_000_000_000, bytes_accessed=2_000_000, transcendentals=0),
    )(plan, *arrays)


def store_kernel(layout, ranks, direct, count, plan, *refs):
    n_data, n_tensor, per_pair = layout.n_data, layout.n_tensor, layout.per_pair
    incoming, probe = refs[:count], refs[count]
    stored, sketch, full, product, places, sems, plan_sem = refs[-7:]
    width = incoming[0].shape[-1]
    slots = len(ranks) * n_tensor
    fetch = pltpu.make_async_copy(plan, places, plan_sem)
    fetch.start()
    copies = []
    begin = 0
    while begin < slots:
        step = min(2, slots - begin)
        for i in range(begin, begin + step):
            k, hop = i // n_tensor, i % n_tensor
            for s in range(n_data):
                if direct:
                    full[i, :, s * width : (s + 1) * width] = incoming[0][s, hop, k]
                else:
                    column = wrap(lax.axis_index("dp") - s + n_data, n_data)
                    columns = pl.ds(pl.multiple_of(column * width, width), width)
                    full[i, :, columns] = incoming[hop][k * n_data + s]
        span = pl.ds(begin, step)
        rows = full[span].reshape(step * BLOCK, n_data * width)
        dot = jnp.dot(rows, probe[...], preferred_element_type=jnp.float32)
        product[span] = dot.reshape(step, BLOCK, probe.shape[1])
        if begin == 0:
            fetch.wait()
        for i in range(begin, begin + step):
            k, u = i // n_tensor, i % n_tensor
            if direct:
                u = wrap(lax.axis_index("tensor") - u + n_tensor, n_tensor)
            slot = places[u * per_pair + ranks[k], per_pair + 1]
            copies.append(pltpu.make_async_copy(full.at[i], stored.at[slot], sems.at[2 * i]))
            copies.append(pltpu.make_async_copy(product.at[i], sketch.at[slot], sems.at[2 * i + 1]))
            copies[-2].start()
            copies[-1].start()
        begin += step
    for copy in copies:
        copy.wait()


def store_ranks(layout, ranks, direct, plan, incoming, probe, previous):
    n_data, n_tensor, per_pair = layout.n_data, layout.n_tensor, layout.per_pair
    count = len(incoming)
    slots = len(ranks) * n_tensor
    columns = n_data * incoming[0].shape[-1]
    sketch_width = probe.shape[1]
    slot_count = n_tensor * per_pair
    out_shape = [
        jax.ShapeDtypeStruct((slot_count, BLOCK, columns), incoming[0].dtype),
        jax.ShapeDtypeStruct((slot_count, BLOCK, sketch_width), jnp.float32),
    ]
    held = [] if previous is None else list(previous)
    return pl.pallas_call(
        functools.partial(store_kernel, layout, ranks, direct, count),
        out_shape=out_shape,
        in_specs=[any_space()] + [vmem()] * (count + 1) + [any_space() for _ in held],
        out_specs=[any_space(), any_space()],
        scratch_shapes=[
            pltpu.VMEM((slots, BLOCK, columns), incoming[0].dtype),
            pltpu.VMEM((slots, BLOCK, sketch_width), jnp.float32),
            pltpu.SMEM(plan.shape, jnp.int32),
            pltpu.SemaphoreType.DMA((2 * slots,)),
            pltpu.SemaphoreType.DMA,
        ],
        compiler_params=pltpu.CompilerParams(vmem_limit_bytes=(8 + 7 * slots // 8) * MIB),
        input_output_aliases={count + 2: 0, count + 3: 1} if held else {},
        cost_estimate=pl.CostEstimate(
            flops=2 * slots * BLOCK * columns * sketch_width,
            bytes_accessed=800_000 * slots,
            transcendentals=0,
        ),
    )(plan, *incoming, probe, *held)


def shards(embed_rows, head_rows, row_offsets, slot_table, probe):
    n_tensor = lax.axis_size("tensor")
    n_data = lax.axis_size("dp")
    quarter = R // 4
    devices = n_tensor * n_data
    per_pair = slot_table.shape[0] // devices // n_tensor
    layout = Layout(n_data, n_tensor, per_pair)

    lead_part, trail_part = cut_edges(row_offsets, embed_rows, head_rows, quarter)
    from_right = from_behind(lead_part, "tensor", -1)
    from_left = from_behind(trail_part, "tensor", 1)
    plan = make_plan(row_offsets, slot_table, n_data, n_tensor, per_pair)

    def move(block, s):
        if s == 0:
            return block
        return from_behind(block, "dp", s)

    def pack_all(arrays, limit):
        return pack(layout, arrays, plan, row_offsets, embed_rows, head_rows, limit)

    def overlay_all(arrays, packed):
        return overlay(layout, arrays, plan, row_offsets, packed, from_left, from_right)

    every_z = range(n_data)

    def send_z(group):
        return [move(group[s], s) for s in every_z]

    ranks = list(range(per_pair - layout.direct_ranks))
    rest = [layout.stage(rank) for rank in ranks[1:]] + [layout.direct()]
    if ranks:
        apart = near_half(n_data)
        whole, first = layout.stage(0), {}
        for shifts in (apart[:1], apart[1:] + [0]):
            first.update(zip(shifts, pack_all([whole[s] for s in shifts], 60)))
        stages = {0: send_z(first)}
        rest = [layout.late() + rest[0]] + rest[1:]
    packed = pack_all([parts for group in rest for parts in group], 50)
    complete, at = [], 0
    for group in rest:
        complete.append(overlay_all(group, packed[at : at + len(group)]))
        at += len(group)
    if ranks:
        late = send_z(complete[0][:n_data])
        for rank in ranks[1:]:
            stages[rank] = send_z(complete[0][n_data * rank :])

        def resend(early):
            return send_z(overlay_all(layout.stage(0), [first[s] for s in every_z]))

        crowded = plan[0, per_pair + 2] > LATE
        stages[0] = lax.cond(crowded, resend, lambda early: early, stages[0])
    direct = lax.all_to_all(
        complete[-1][0], ("dp", "tensor"), split_axis=0, concat_axis=0, tiled=True
    )
    direct = direct.reshape((n_data, n_tensor, layout.direct_ranks) + direct.shape[1:])
    outputs = None
    for rank in ranks:
        arrays = stages[rank] + (late if rank == 0 else [])
        gathered = gather_forward(layout, [rank], plan, arrays)
        forwarded = [gathered[0]]
        for u in range(1, n_tensor):
            forwarded.append(from_behind(gathered[u], "tensor", u))
        outputs = store_ranks(layout, [rank], False, plan, forwarded, probe, outputs)
    last = list(range(per_pair - layout.direct_ranks, per_pair))
    return tuple(store_ranks(layout, last, True, plan, [direct], probe, outputs))


def near_half(n_data):
    return sorted(range(1, n_data), key=lambda s: (abs(2 * s - n_data), s))


def solution(mesh):
    return jax.shard_map(
        shards,
        mesh=mesh,
        in_specs=(P("tensor", "dp"), P("tensor", "dp"), P(), P(), P()),
        out_specs=(P(("dp", "tensor"), None, None), P(("dp", "tensor"), None, None)),
        check_vma=False,
    )
```

```python
import functools

import jax
import jax.numpy as jnp
from jax import lax
from jax.experimental import pallas as pl
from jax.experimental.pallas import tpu as pltpu
from jax.sharding import PartitionSpec as P


R = 8192
BLOCK = 128
LATE = 1
DIRECT = 2
ALIGN = 16
MIB = 1 << 20


def from_behind(block, axis, distance):
    devices = range(lax.axis_size(axis))
    route = [((i - distance) % len(devices), i) for i in devices]
    return lax.ppermute(block, axis, route)


def any_space():
    return pl.BlockSpec(memory_space=pl.ANY)


def in_hbm():
    return pl.BlockSpec(memory_space=pltpu.HBM)


def smem():
    return pl.BlockSpec(memory_space=pltpu.SMEM)


def vmem():
    return pl.BlockSpec(memory_space=pltpu.VMEM)


def my_span(offsets, m):
    t = lax.axis_index("tensor")
    return offsets[m, t] - t * R, offsets[m, t + 1] - t * R


def edges_kernel(offsets, embed, head, lead_out, trail_out, lead_in, trail_in, sems, out_sems):
    quarter = lead_out.shape[1]
    copies = []
    writes = []
    for m, raw in enumerate([embed, head]):
        first = (R - my_span(offsets, m)[0]) & -ALIGN
        window = pl.ds(pl.multiple_of(first, ALIGN), quarter + ALIGN)
        copies.append(
            pltpu.make_async_copy(raw.at[pl.ds(0, quarter)], lead_in.at[m], sems.at[2 * m])
        )
        copies.append(pltpu.make_async_copy(raw.at[window], trail_in.at[m], sems.at[2 * m + 1]))
        writes.append(pltpu.make_async_copy(lead_in.at[m], lead_out.at[m], out_sems.at[2 * m]))
        writes.append(pltpu.make_async_copy(trail_in.at[m], trail_out.at[m], out_sems.at[2 * m + 1]))
    for copy in copies:
        copy.start()
    for copy, write in zip(copies, writes):
        copy.wait()
        write.start()
    for write in writes:
        write.wait()


def cut_edges(offsets, embed, head, quarter):
    width = embed.shape[1]
    return pl.pallas_call(
        edges_kernel,
        out_shape=[
            jax.ShapeDtypeStruct((2, rows, width), embed.dtype) for rows in (quarter, quarter + ALIGN)
        ],
        in_specs=[smem(), in_hbm(), in_hbm()],
        out_specs=[in_hbm()] * 2,
        scratch_shapes=[
            pltpu.VMEM((2, quarter, width), embed.dtype),
            pltpu.VMEM((2, quarter + ALIGN, width), embed.dtype),
            pltpu.SemaphoreType.DMA((4,)),
            pltpu.SemaphoreType.DMA((4,)),
        ],
        compiler_params=pltpu.CompilerParams(vmem_limit_bytes=61 * MIB),
    )(offsets, embed, head)


def log2(size):
    assert size & (size - 1) == 0
    return size.bit_length() - 1


def wrap(index, size):
    return index & (size - 1)


def target(s, u, n_data, n_tensor):
    z = wrap(lax.axis_index("dp") + s, n_data)
    t = wrap(lax.axis_index("tensor") + u, n_tensor)
    return z * n_tensor + t


def split_block(block):
    bits = log2(R // BLOCK)
    return block >> bits, (block & (R // BLOCK - 1)) * BLOCK


def plan_kernel(n_data, n_tensor, per_pair, offsets, slots, plan):
    devices, count = slots.shape
    per_rank = R // BLOCK
    total = per_rank * n_tensor
    slot = slots[...]
    matrix = slot >> log2(total)
    rest = slot & (total - 1)
    source = rest >> log2(per_rank)
    k = rest & (per_rank - 1)
    local = jnp.zeros_like(slot)
    for m in range(2):
        for t in range(n_tensor):
            begin = offsets[m, t] - t * R
            end = offsets[m, t + 1] - t * R
            inside = (k * BLOCK >= begin) & (k * BLOCK + BLOCK <= end)
            here = (source == t) & (matrix == m)
            local = jnp.where(here & inside, 1, local)
    column = lax.broadcasted_iota(jnp.int32, slot.shape, 1)
    lowest = source * (2 * count)
    key = lowest + (1 - local) * count + column
    rank = jnp.zeros_like(slot)
    for j in range(count):
        other = key[:, j : j + 1]
        rank += jnp.where((other >= lowest) & (other < key), 1, 0)
    my_t = lax.axis_index("tensor")
    me = lax.axis_index("dp") * n_tensor + my_t
    lane = lax.broadcasted_iota(jnp.int32, plan.shape, 1)
    row = lax.broadcasted_iota(jnp.int32, slot.shape, 0)
    out = jnp.zeros(plan.shape, jnp.int32)
    block = matrix * per_rank + k
    for r in range(per_pair):
        mine = (source == my_t) & (rank == r)
        picked = jnp.sum(jnp.where(mine, block, 0), axis=1, keepdims=True)
        out = jnp.where(lane == r, picked, out)
        if r == 0:
            flag = jnp.sum(jnp.where(mine, local, 0), axis=1, keepdims=True)
            out = jnp.where(lane == per_pair, flag, out)
    hops = (my_t - source) & (n_tensor - 1)
    order = jnp.where(row == me, hops * per_pair + rank, 0)
    order = jnp.sum(order, axis=0, keepdims=True)
    found = jnp.where(order == row, column, 0)
    out = jnp.where(lane == per_pair + 1, jnp.sum(found, axis=1, keepdims=True), out)
    empty = jnp.zeros(plan.shape, jnp.int32)
    for t in range(n_tensor):
        has = jnp.max(jnp.where(source == t, local, 0), axis=1, keepdims=True)
        empty = jnp.where(lane == t, 1 - has, empty)
    worst = jnp.zeros((1, 1), jnp.int32)
    for z in range(n_data):
        layer = jnp.sum(empty[z * n_tensor : (z + 1) * n_tensor], axis=0, keepdims=True)
        worst = jnp.maximum(worst, jnp.max(layer, axis=1, keepdims=True))
    plan[...] = jnp.where(lane == per_pair + 2, worst, out)


def make_plan(offsets, slot_table, n_data, n_tensor, per_pair):
    devices = n_data * n_tensor
    return pl.pallas_call(
        functools.partial(plan_kernel, n_data, n_tensor, per_pair),
        out_shape=jax.ShapeDtypeStruct((devices, 128), jnp.int32),
        in_specs=[smem(), vmem()],
        out_specs=vmem(),
        compiler_params=pltpu.CompilerParams(vmem_limit_bytes=4 * MIB),
    )(offsets, slot_table.reshape(devices, -1))


class Layout:
    def __init__(self, n_data, n_tensor, per_pair):
        self.n_data, self.n_tensor, self.per_pair = n_data, n_tensor, per_pair
        self.staged = per_pair > DIRECT + 1
        self.direct_ranks = DIRECT if self.staged else per_pair

    def target(self, s, u):
        return target(s, u, self.n_data, self.n_tensor)

    def along_z(self, s, rank):
        return (0, self.n_tensor, lambda plan, i: plan[self.target(s, i), rank])

    def late_block(self, plan, s):
        chosen = self.target(s, 0)
        for u in reversed(range(self.n_tensor)):
            to = self.target(s, u)
            chosen = jnp.where(plan[to, self.per_pair] == 0, to, chosen)
        return plan[chosen, 0]

    def late(self):
        return [
            [(0, LATE, lambda plan, i, s=s: self.late_block(plan, s))] for s in range(self.n_data)
        ]

    def stage(self, rank):
        return [[self.along_z(s, rank)] for s in range(self.n_data)]

    def direct(self):
        count, first = self.direct_ranks, self.per_pair - self.direct_ranks
        bits = log2(count)
        which = lambda plan, i: plan[i >> bits, first + (i & (count - 1))]
        return [[(0, self.n_data * self.n_tensor * count, which)]]

    def size(self, parts):
        return sum(part[1] for part in parts)


def pack_kernel(arrays, plan, offsets, embed, head, *refs):
    outs, (windows, wide, sems) = refs[: len(arrays)], refs[len(arrays) :]
    height = embed.shape[0]

    t = lax.axis_index("tensor")
    begins = [offsets[m, t] - t * R for m in range(2)]

    def where_from(block):
        m, row = split_block(block)
        start = row - jnp.where(m == 0, begins[0], begins[1])
        start = jnp.minimum(jnp.maximum(start + BLOCK, 0), height - ALIGN)
        first = jnp.maximum((start & -ALIGN) - BLOCK, 0)
        return m, start - BLOCK, pl.multiple_of(first, ALIGN)

    at = 0
    for parts in arrays:
        for begin, count, which in parts:

            def fetch(i, _, at=at, which=which):
                m, _start, first = where_from(which(plan, i))
                for k, raw in enumerate([embed, head]):

                    @pl.when(m == k)
                    def _fetch(raw=raw):
                        pltpu.make_async_copy(
                            raw.at[pl.ds(first, BLOCK + ALIGN)], windows.at[at + i], sems.at[at + i]
                        ).start()

                return _

            lax.fori_loop(0, count, fetch, 0)
            at += count
    at = 0
    for parts, out in zip(arrays, outs):
        for begin, count, which in parts:

            def shift(i, _, at=at, which=which, out=out, begin=begin):
                m, start, first = where_from(which(plan, i))
                pltpu.make_async_copy(
                    embed.at[pl.ds(0, BLOCK + ALIGN)], windows.at[at + i], sems.at[at + i]
                ).wait()
                slot = i & 1
                wide[slot, pl.ds(BLOCK, BLOCK + ALIGN), :] = windows[at + i].astype(jnp.float32)
                moved = wide[slot, pl.ds(BLOCK + start - first, BLOCK), :]
                out[begin + i] = moved.astype(jnp.bfloat16)
                return _

            lax.fori_loop(0, count, shift, 0)
            at += count


def pack(layout, arrays, plan, offsets, embed, head, limit):
    width = embed.shape[1]
    total = sum(layout.size(parts) for parts in arrays)
    return pl.pallas_call(
        functools.partial(pack_kernel, arrays),
        out_shape=[
            jax.ShapeDtypeStruct((layout.size(parts), BLOCK, width), embed.dtype) for parts in arrays
        ],
        in_specs=[smem(), smem(), in_hbm(), in_hbm()],
        out_specs=[vmem()] * len(arrays),
        scratch_shapes=[
            pltpu.VMEM((total, BLOCK + ALIGN, width), embed.dtype),
            pltpu.VMEM((2, 2 * BLOCK + ALIGN, width), jnp.float32),
            pltpu.SemaphoreType.DMA((total,)),
        ],
        compiler_params=pltpu.CompilerParams(vmem_limit_bytes=limit * MIB),
        cost_estimate=pl.CostEstimate(flops=total * 30_000_000, bytes_accessed=total * 70_000, transcendentals=0),
    )(plan, offsets, embed, head)


def overlay_kernel(arrays, n_tensor, plan, offsets, *refs):
    count = len(arrays)
    packed, left, right, outs, wide = refs[:count], refs[count], refs[count + 1], refs[-count - 1 : -1], refs[-1]
    quarter = right.shape[1]
    t = lax.axis_index("tensor")
    begins = [offsets[m, t] - t * R for m in range(2)]
    ends = [offsets[m, t + 1] - t * R for m in range(2)]
    behind = wrap(t + n_tensor - 1, n_tensor)
    shifts = [(R - offsets[m, behind] + behind * R) & (ALIGN - 1) for m in range(2)]
    for parts, source, out in zip(arrays, packed, outs):
        out[...] = source[...]
        for begin, blocks, which in parts:

            def fix(i, _, begin=begin, which=which, out=out):
                m, first = split_block(which(plan, i))
                before = jnp.where(m == 0, begins[0], begins[1])
                after = jnp.where(m == 0, ends[0], ends[1])

                @pl.when((first < before) | (first + BLOCK > after))
                def _edge():
                    @pl.when(first < before)
                    def _left():
                        row = first + lax.broadcasted_iota(jnp.int32, (BLOCK, 1), 0)
                        window = pl.ds(pl.multiple_of(first, BLOCK), BLOCK + ALIGN)
                        wide[pl.ds(0, BLOCK + ALIGN), :] = left[m, window, :].astype(jnp.float32)
                        shift = jnp.where(m == 0, shifts[0], shifts[1])
                        edge = wide[pl.ds(shift, BLOCK), :].astype(out.dtype)
                        out[begin + i] = jnp.where(row < before, edge, out[begin + i])

                    @pl.when(first + BLOCK > after)
                    def _right():
                        row = first + lax.broadcasted_iota(jnp.int32, (BLOCK, 1), 0)
                        start = first - after
                        at = jnp.clip(start & -ALIGN, 0, quarter - BLOCK - ALIGN)
                        window = pl.ds(pl.multiple_of(at, ALIGN), BLOCK + ALIGN)
                        wide[pl.ds(BLOCK, BLOCK + ALIGN), :] = right[m, window, :].astype(jnp.float32)
                        edge = wide[pl.ds(BLOCK + start - at, BLOCK), :].astype(out.dtype)
                        out[begin + i] = jnp.where(row >= after, edge, out[begin + i])

                return _

            lax.fori_loop(0, blocks, fix, 0)


def overlay(layout, arrays, plan, offsets, packed, left, right):
    return pl.pallas_call(
        functools.partial(overlay_kernel, arrays, layout.n_tensor),
        out_shape=[
            jax.ShapeDtypeStruct((layout.size(parts),) + packed[0].shape[1:], left.dtype)
            for parts in arrays
        ],
        in_specs=[smem()] * 2 + [vmem()] * (len(packed) + 2),
        out_specs=[vmem()] * len(arrays),
        scratch_shapes=[pltpu.VMEM((2 * BLOCK + ALIGN, packed[0].shape[2]), jnp.float32)],
        compiler_params=pltpu.CompilerParams(vmem_limit_bytes=16 * MIB),
        cost_estimate=pl.CostEstimate(flops=1_000_000_000, bytes_accessed=4_000_000, transcendentals=0),
    )(plan, offsets, *packed, left, right)


def forward_kernel(layout, ranks, plan, *refs):
    n_data, n_tensor, per_pair = layout.n_data, layout.n_tensor, layout.per_pair
    outs = refs[-n_tensor:]
    for u in range(n_tensor):
        to = layout.target(0, u)
        swap = (plan[to, per_pair] == 0) & (plan[0, per_pair + 2] <= LATE)
        for k, rank in enumerate(ranks):
            for s in range(n_data):
                if rank == 0:

                    @pl.when(swap)
                    def _late(s=s, u=u):
                        outs[u][s] = refs[n_data + s][0]

                    @pl.when(jnp.logical_not(swap))
                    def _early(s=s, u=u):
                        outs[u][s] = refs[s][u]

                else:
                    outs[u][k * n_data + s] = refs[k * n_data + s][u]


def gather_forward(layout, ranks, plan, arrays):
    n_tensor = layout.n_tensor
    _, _, width = arrays[0].shape
    shape = jax.ShapeDtypeStruct((len(ranks) * layout.n_data, BLOCK, width), arrays[0].dtype)
    return pl.pallas_call(
        functools.partial(forward_kernel, layout, ranks),
        out_shape=[shape] * n_tensor,
        in_specs=[smem()] + [vmem()] * len(arrays),
        out_specs=[vmem()] * n_tensor,
        compiler_params=pltpu.CompilerParams(vmem_limit_bytes=12 * MIB),
        cost_estimate=pl.CostEstimate(flops=1_000_000_000, bytes_accessed=2_000_000, transcendentals=0),
    )(plan, *arrays)


def store_kernel(layout, ranks, direct, count, plan, *refs):
    n_data, n_tensor, per_pair = layout.n_data, layout.n_tensor, layout.per_pair
    incoming, probe = refs[:count], refs[count]
    stored, sketch, full, product, places, sems, plan_sem = refs[-7:]
    width = incoming[0].shape[-1]
    slots = len(ranks) * n_tensor
    fetch = pltpu.make_async_copy(plan, places, plan_sem)
    fetch.start()
    copies = []
    begin = 0
    while begin < slots:
        step = min(2, slots - begin)
        for i in range(begin, begin + step):
            k, hop = i // n_tensor, i % n_tensor
            for s in range(n_data):
                if direct:
                    full[i, :, s * width : (s + 1) * width] = incoming[0][s, hop, k]
                else:
                    column = wrap(lax.axis_index("dp") - s + n_data, n_data)
                    columns = pl.ds(pl.multiple_of(column * width, width), width)
                    full[i, :, columns] = incoming[hop][k * n_data + s]
        span = pl.ds(begin, step)
        rows = full[span].reshape(step * BLOCK, n_data * width)
        dot = jnp.dot(rows, probe[...], preferred_element_type=jnp.float32)
        product[span] = dot.reshape(step, BLOCK, probe.shape[1])
        if begin == 0:
            fetch.wait()
        for i in range(begin, begin + step):
            k, u = i // n_tensor, i % n_tensor
            if direct:
                u = wrap(lax.axis_index("tensor") - u + n_tensor, n_tensor)
            slot = places[u * per_pair + ranks[k], per_pair + 1]
            copies.append(pltpu.make_async_copy(full.at[i], stored.at[slot], sems.at[2 * i]))
            copies.append(pltpu.make_async_copy(product.at[i], sketch.at[slot], sems.at[2 * i + 1]))
            copies[-2].start()
            copies[-1].start()
        begin += step
    for copy in copies:
        copy.wait()


def store_ranks(layout, ranks, direct, plan, incoming, probe, previous):
    n_data, n_tensor, per_pair = layout.n_data, layout.n_tensor, layout.per_pair
    count = len(incoming)
    slots = len(ranks) * n_tensor
    columns = n_data * incoming[0].shape[-1]
    sketch_width = probe.shape[1]
    slot_count = n_tensor * per_pair
    out_shape = [
        jax.ShapeDtypeStruct((slot_count, BLOCK, columns), incoming[0].dtype),
        jax.ShapeDtypeStruct((slot_count, BLOCK, sketch_width), jnp.float32),
    ]
    held = [] if previous is None else list(previous)
    return pl.pallas_call(
        functools.partial(store_kernel, layout, ranks, direct, count),
        out_shape=out_shape,
        in_specs=[any_space()] + [vmem()] * (count + 1) + [any_space() for _ in held],
        out_specs=[any_space(), any_space()],
        scratch_shapes=[
            pltpu.VMEM((slots, BLOCK, columns), incoming[0].dtype),
            pltpu.VMEM((slots, BLOCK, sketch_width), jnp.float32),
            pltpu.SMEM(plan.shape, jnp.int32),
            pltpu.SemaphoreType.DMA((2 * slots,)),
            pltpu.SemaphoreType.DMA,
        ],
        compiler_params=pltpu.CompilerParams(vmem_limit_bytes=(8 + 7 * slots // 8) * MIB),
        input_output_aliases={count + 2: 0, count + 3: 1} if held else {},
        cost_estimate=pl.CostEstimate(
            flops=2 * slots * BLOCK * columns * sketch_width,
            bytes_accessed=800_000 * slots,
            transcendentals=0,
        ),
    )(plan, *incoming, probe, *held)


def shards(embed_rows, head_rows, row_offsets, slot_table, probe):
    n_tensor = lax.axis_size("tensor")
    n_data = lax.axis_size("dp")
    quarter = R // 4
    devices = n_tensor * n_data
    per_pair = slot_table.shape[0] // devices // n_tensor
    layout = Layout(n_data, n_tensor, per_pair)

    lead_part, trail_part = cut_edges(row_offsets, embed_rows, head_rows, quarter)
    from_right = from_behind(lead_part, "tensor", -1)
    from_left = from_behind(trail_part, "tensor", 1)
    plan = make_plan(row_offsets, slot_table, n_data, n_tensor, per_pair)

    def move(block, s):
        if s == 0:
            return block
        return from_behind(block, "dp", s)

    def pack_all(arrays, limit):
        return pack(layout, arrays, plan, row_offsets, embed_rows, head_rows, limit)

    def overlay_all(arrays, packed):
        return overlay(layout, arrays, plan, row_offsets, packed, from_left, from_right)

    every_z = range(n_data)

    def send_z(group):
        return [move(group[s], s) for s in every_z]

    ranks = list(range(per_pair - layout.direct_ranks))
    rest = [layout.stage(rank) for rank in ranks[1:]] + [layout.direct()]
    if ranks:
        apart = near_half(n_data)
        whole, first = layout.stage(0), {}
        for shifts in (apart[:1], apart[1:]):
            first.update(zip(shifts, pack_all([whole[s] for s in shifts], 60)))
        late, one = layout.late(), rest[0]
        sent = [late[s] for s in apart] + [one[s] for s in apart]
        rest = [sent] + rest[1:-1] + [rest[-1] + [late[0], one[0]]]
    own = [whole[0]] if ranks else []
    packed = pack_all([parts for group in rest for parts in group] + own, 50)
    complete, at = [], 0
    for group in rest:
        complete.append(overlay_all(group, packed[at : at + len(group)]))
        at += len(group)
    if ranks:
        first[0] = packed[at]
        stages = {0: send_z(first)}
        count = len(apart)
        late = send_z(dict(zip(apart + [0], complete[0][:count] + complete[-1][1:2])))
        one = dict(zip(apart + [0], complete[0][count:] + complete[-1][2:3]))
        stages[1] = send_z(one)
        for rank in ranks[2:]:
            stages[rank] = send_z(complete[rank - 1])

        def resend(early):
            again = overlay_all(layout.stage(0), [first[s] for s in every_z])
            return send_z(again)

        crowded = plan[0, per_pair + 2] > LATE
        stages[0] = lax.cond(crowded, resend, lambda early: early, stages[0])
    direct = lax.all_to_all(
        complete[-1][0], ("dp", "tensor"), split_axis=0, concat_axis=0, tiled=True
    )
    direct = direct.reshape((n_data, n_tensor, layout.direct_ranks) + direct.shape[1:])
    outputs = None
    for rank in ranks:
        arrays = stages[rank] + (late if rank == 0 else [])
        gathered = gather_forward(layout, [rank], plan, arrays)
        forwarded = [gathered[0]]
        for u in range(1, n_tensor):
            forwarded.append(from_behind(gathered[u], "tensor", u))
        outputs = store_ranks(layout, [rank], False, plan, forwarded, probe, outputs)
    last = list(range(per_pair - layout.direct_ranks, per_pair))
    return tuple(store_ranks(layout, last, True, plan, [direct], probe, outputs))


def near_half(n_data):
    return sorted(range(1, n_data), key=lambda s: (abs(2 * s - n_data), s))


def solution(mesh):
    return jax.shard_map(
        shards,
        mesh=mesh,
        in_specs=(P("tensor", "dp"), P("tensor", "dp"), P(), P(), P()),
        out_specs=(P(("dp", "tensor"), None, None), P(("dp", "tensor"), None, None)),
        check_vma=False,
    )
```
